32 devices in a mesh: feed: 8 (over y, x, core), band: 4 (over z).
Axes of the slice: x: 2, y: 2, z: 4, core: 2. Of those that a mesh axis runs over, the one named last changes fastest.
Arguments:
- voltages: int32 [4, 8, 1024, 512], P('band', None, 'feed'), may hold values from -2147483648 to 2147483646
- complex_gains: float32 [2, 4, 8, 1024], P(None, 'band', None, 'feed'), may hold values from -4 to 4
- channel_map: int32 [4, 8], P('band'), may hold values from 0 to 7, each once within a row
Outputs:
- visibility: float32 [2, 4, 8, 1024, 1024], P(None, 'band', 'feed')
The draws below stay inside these ranges and needn't reach their ends.
Inputs may be any that keep to these rules, and one draw needn't show every extreme that they name: `channel_map`: each sub-band's row is a permutation of 0 to 7.
All inputs are finite; a program needn't handle non-finite values.
Results may differ from the reference program's by a relative error of at most 0.0003.
Values sent between devices are 32-bit elements; how exact they have to be, the bound alone decides.
A program may use at most 128 MiB of HBM per device.

```python
import jax
import jax.numpy as jnp
from jax import lax

F = 1024
T_SAMPLES = 2048
TW = 512
CHB = 8
N_BAND = 4


def touch_ends(drawn, rng, least, largest):
    longest = drawn.shape.index(max(drawn.shape))
    spots = []
    for shift in (0, 1):
        where = [jax.random.randint(jax.random.fold_in(rng, axis), (), 0, length) for axis, length in enumerate(drawn.shape)]
        where[longest] = (where[longest] + shift) % drawn.shape[longest]
        spots.append(tuple(where))
    return drawn.at[spots[0]].set(least).at[spots[1]].set(largest)


def levels(rng, dims, split, smallest, top_value):
    loudness = 1.0
    for axis_at, parts in split:
        heights = jax.random.uniform(jax.random.fold_in(jax.random.fold_in(rng, 6), axis_at), (parts,), jnp.float32, smallest / len(split), top_value / len(split))
        loudness = loudness * jnp.repeat(jnp.exp(heights), dims[axis_at] // parts).reshape((-1,) + (1,) * (len(dims) - 1 - axis_at))
    return loudness


def centred(rng, dims, spread, limit, split=(), kind=jnp.bfloat16):
    factor_of = levels(rng, dims, split, -0.22, 0.18) if split else 1.0
    entries = jax.random.normal(rng, dims, jnp.float32) * spread * factor_of
    return jnp.minimum(jnp.maximum(entries, -limit), limit).astype(kind)


def setup_inputs(seed: int = 0) -> dict:
    keys = jax.random.split(jax.random.key(seed), 4)
    return {
        "voltages": touch_ends(jax.random.randint(keys[0], (N_BAND, CHB, F, TW), -2147483648, 2147483647), jax.random.fold_in(keys[0], 1), -2147483648, 2147483646).astype(jnp.int32),
        "complex_gains": centred(keys[1], (2, N_BAND, CHB, F), 1.0, 4.0, ((1, 4), (3, 8)), jnp.float32),
        "channel_map": jax.vmap(lambda own: jax.random.permutation(own, CHB))(jax.random.split(keys[2], N_BAND)).reshape((N_BAND, CHB)).astype(jnp.int32),
    }


def unpack_samples(packed):
    shifts = jnp.arange(4, dtype=jnp.int32) * 8
    fields = jnp.right_shift(packed[..., None], shifts)
    real_part = jnp.bitwise_xor(jnp.bitwise_and(fields, 15), 8) - 8
    imag_part = jnp.bitwise_xor(jnp.bitwise_and(jnp.right_shift(fields, 4), 15), 8) - 8
    leading = packed.shape[:-1]
    real_part = real_part.reshape(leading + (packed.shape[-1] * 4,)).astype(jnp.bfloat16)
    imag_part = imag_part.reshape(leading + (packed.shape[-1] * 4,)).astype(jnp.bfloat16)
    return real_part, imag_part


def reference(voltages, complex_gains, channel_map):
    scale = 1.0 / (16.0 * T_SAMPLES)

    def one_slot(flat):
        band_index = flat // CHB
        slot_index = flat % CHB
        channel = channel_map[band_index, slot_index]
        packed = voltages[band_index, channel]
        gain_re = complex_gains[0, band_index, channel]
        gain_im = complex_gains[1, band_index, channel]
        real_part, imag_part = unpack_samples(packed)
        stacked = jnp.concatenate([real_part, imag_part], axis=1)
        rotated = jnp.concatenate([imag_part, -real_part], axis=1)
        gram_re = jnp.dot(stacked, stacked.T, preferred_element_type=jnp.float32)
        gram_im = jnp.dot(rotated, stacked.T, preferred_element_type=jnp.float32)
        weight_re = gain_re[:, None] * gain_re[None, :] + gain_im[:, None] * gain_im[None, :]
        weight_im = gain_im[:, None] * gain_re[None, :] - gain_re[:, None] * gain_im[None, :]
        vis_re = (weight_re * gram_re - weight_im * gram_im) * scale
        vis_im = (weight_re * gram_im + weight_im * gram_re) * scale
        return vis_re, vis_im

    flat = jnp.arange(N_BAND * CHB, dtype=jnp.int32)
    vis_re, vis_im = lax.map(one_slot, flat)
    return jnp.stack([vis_re, vis_im]).reshape(2, N_BAND, CHB, F, F)
```

```python
import functools

import jax
import jax.numpy as jnp
from jax import lax
from jax.experimental import pallas as pl
from jax.experimental.pallas import tpu as pltpu
from jax.sharding import PartitionSpec as P

MESH = pl.DeviceIdType.MESH
PLANE = jnp.bfloat16
BLOCK = 128
LANES = 128


def flip(index, mask, size):
    total, bit = 0, 1
    while bit < size:
        digit = lax.rem(index // bit, 2)
        total = total + ((1 - digit) if mask & bit else digit) * bit
        bit *= 2
    return total


def weigh(gram, col, row):
    gram_re = gram[:BLOCK, :BLOCK] + gram[BLOCK:, BLOCK:]
    gram_im = gram[BLOCK:, :BLOCK] - gram[:BLOCK, BLOCK:]
    col_re, col_im = col[:, 0:1], col[:, 1:2]
    row_re, row_im = row[0:1, :], row[1:2, :]
    weight_re = col_re * row_re + col_im * row_im
    weight_im = col_im * row_re - col_re * row_im
    return weight_re * gram_re - weight_im * gram_im, weight_re * gram_im + weight_im * gram_re


def product(left, right):
    return lax.dot_general(left, right, (((1,), (1,)), ((), ())), preferred_element_type=jnp.float32)


def send_order(n):
    return sorted(range(1, n), key=lambda m: (m & (m - 1) > 1 and bin(m >> 1).count("1") > 1, m & 1, m))


def group_order(n, per_group):
    seen = []
    for mask in [0] + send_order(n):
        if mask // per_group not in seen:
            seen.append(mask // per_group)
    return seen


def gather_kernel(n, scale, map_hbm, volt_hbm, gain_hbm, vis_ref, planes, acc, gcols, grows,
                  map_ref, gain_ref, volts, stage, gstage, recv, grecv,
                  map_sem, gain_sem, load_sem, send_sem, recv_sem, gsend_sem, grecv_sem):
    me = lax.axis_index("feed")
    rows, words = stage.shape[1], stage.shape[2]
    per_group = BLOCK // rows
    groups = n // per_group
    chunks = words // LANES
    low = lax.rem(me, per_group)
    own_group = me // per_group
    arrivals = group_order(n, per_group)
    whole, chunked = arrivals[:-2], arrivals[-2:]
    last = chunked[-1]
    pieces = len(volts)
    step = rows // pieces

    map_copy = pltpu.make_async_copy(map_hbm, map_ref, map_sem)
    gain_copy = pltpu.make_async_copy(gain_hbm, gain_ref, gain_sem)
    loads = []
    for p in range(pieces):
        strip = pl.ds(p * step, step)
        loads.append(pltpu.make_async_copy(volt_hbm.at[0, :, strip], volts[p], load_sem.at[p]))
    map_copy.start()
    for load in loads:
        load.start()
    gain_copy.start()
    barrier = pltpu.get_barrier_semaphore()
    for mask in range(1, n):
        pl.semaphore_signal(barrier, inc=1, device_id={"feed": flip(me, mask, n)}, device_id_type=MESH)
    map_copy.wait()
    order = send_order(n)
    lead, rest = order[:2], order[2:]
    copies = []

    def send(source, target, sent, landed, mask):
        copies.append(pltpu.make_async_remote_copy(
            src_ref=source, dst_ref=target, send_sem=sent, recv_sem=landed,
            device_id={"feed": flip(me, mask, n)}, device_id_type=MESH))
        copies[-1].start()

    def spot(mask):
        return (mask // per_group) * per_group + low

    for p in range(pieces):
        strip = pl.ds(p * step, step)
        loads[p].wait()
        for mask in lead:
            stage[mask, strip] = volts[p][map_ref[0, flip(me, mask, n)]]
        if p == 0:
            pl.semaphore_wait(barrier, n - 1)
        for mask in lead:
            send(stage.at[mask, strip], recv.at[spot(mask), strip], send_sem.at[mask, p],
                 recv_sem.at[spot(mask), p], mask)
    for mask in rest:
        for p in range(pieces):
            stage[mask, pl.ds(p * step, step)] = volts[p][map_ref[0, flip(me, mask, n)]]
        if mask // per_group in whole:
            send(stage.at[mask], recv.at[spot(mask)], send_sem.at[mask, 0], recv_sem.at[spot(mask), 0], mask)
    gain_copy.wait()
    for mask in range(n):
        channel = map_ref[0, flip(me, mask, n)]
        for part in range(2):
            gstage[mask, part:part + 1, :] = gain_ref[part, pl.ds(channel, 1), :]
    for mask in order:
        send(gstage.at[mask], grecv.at[spot(mask)], gsend_sem.at[mask], grecv_sem.at[spot(mask)], mask)
    for group in chunked:
        for c in range(chunks):
            part = pl.ds(c * LANES, LANES)
            for mask in rest:
                if mask // per_group == group:
                    send(stage.at[mask, :, part], recv.at[spot(mask), :, part], send_sem.at[mask, c],
                         recv_sem.at[spot(mask), c], mask)
    for p in range(pieces):
        recv[low, pl.ds(p * step, step)] = volts[p][map_ref[0, me]]
    grecv[low] = gstage[0]

    def places(group):
        return [group * per_group + flip(low, t, per_group) for t in range(per_group) if group or t]

    def arrive(group):
        for t in range(per_group):
            place = group * per_group + flip(low, t, per_group)
            if group * per_group + t in lead:
                for p in range(pieces):
                    here = recv.at[place, pl.ds(p * step, step)]
                    pltpu.make_async_copy(here, here, recv_sem.at[place, p]).wait()
            elif group or t:
                pltpu.make_async_copy(recv.at[place], recv.at[place], recv_sem.at[place, 0]).wait()

    def unpack(group, c):
        step = 32
        part_of = pl.ds(c * LANES, LANES)

        def piece(i, carry):
            start = pl.multiple_of(i * step, step)
            if rows >= step:
                packed = recv[group, pl.ds(start, step), part_of]
            else:
                first = group * per_group + i * (step // rows)
                packed = recv[pl.ds(first, step // rows), :, part_of].reshape(step, LANES)
            for k in range(4):
                for part in range(2):
                    field = jnp.right_shift(jnp.left_shift(packed, 28 - 8 * k - 4 * part), 28)
                    column = (4 * c + k) * LANES
                    planes[group, pl.ds(part * BLOCK + start, step), column:column + LANES] = (
                        field.astype(jnp.float32).astype(PLANE))
            return carry

        lax.fori_loop(0, BLOCK // step, piece, 0)

    def emit(group, other, gram):
        top = pl.multiple_of(flip(own_group, group, groups) * BLOCK, BLOCK)
        left = pl.multiple_of(flip(own_group, other, groups) * BLOCK, BLOCK)
        vis_re, vis_im = weigh(gram, gcols[group], grows[other])
        vis_ref[0, pl.ds(top, BLOCK), pl.ds(left, BLOCK)] = vis_re
        vis_ref[1, pl.ds(top, BLOCK), pl.ds(left, BLOCK)] = vis_im
        if other != group:
            vis_ref[0, pl.ds(left, BLOCK), pl.ds(top, BLOCK)] = jnp.transpose(vis_re)
            vis_ref[1, pl.ds(left, BLOCK), pl.ds(top, BLOCK)] = jnp.transpose(-vis_im)

    for group in range(groups):
        for place in places(group):
            pltpu.make_async_copy(grecv.at[place], grecv.at[place], grecv_sem.at[place]).wait()
        gains = grecv[group * per_group]
        for t in range(1, per_group):
            gains = gains + grecv[group * per_group + t]
        grows[group] = gains
        gcols[group] = jnp.transpose(jnp.concatenate([gains * scale] + [jnp.zeros_like(gains)] * 3, axis=0))

    for position, group in enumerate(whole):
        arrive(group)
        for c in range(chunks):
            unpack(group, c)
        for other in whole[:position + 1]:
            emit(group, other, product(planes[group], planes[other]))

    for group in chunked:
        others = arrivals[:arrivals.index(group) + 1]
        for c in range(chunks):
            for place in places(group):
                here = recv.at[place, :, pl.ds(c * LANES, LANES)]
                pltpu.make_async_copy(here, here, recv_sem.at[place, c]).wait()
            unpack(group, c)
            span = pl.ds(4 * c * LANES, 4 * LANES)
            if c < chunks - 1 or group != last:
                for other in others:
                    term = product(planes[group, :, span], planes[other, :, span])
                    gram = term if c == 0 else acc[other] + term
                    if c < chunks - 1:
                        acc[other] = gram
                    else:
                        emit(group, other, gram)

    for copy in copies:
        copy.wait_send()


def write_kernel(vis_ref, planes, acc, gcols, grows, out_hbm, gram, row_strip, column_strip, sems):
    groups = planes.shape[0]
    per_group = lax.axis_size("feed") // groups
    own_group = lax.axis_index("feed") // per_group
    last = group_order(lax.axis_size("feed"), per_group)[-1]
    span = pl.ds(planes.shape[2] - 4 * LANES, 4 * LANES)

    def spot(group):
        return pl.ds(pl.multiple_of(flip(own_group, group, groups) * BLOCK, BLOCK), BLOCK)

    copies = []

    def write(source, rows, columns):
        copies.append(pltpu.make_async_copy(source, out_hbm.at[:, rows, columns], sems.at[len(copies)]))
        copies[-1].start()

    for group in range(groups):
        if group == last:
            continue
        size = groups // 2
        while size:
            prefix = last // size * size ^ size
            start = flip(own_group, prefix, groups) // size * size
            columns = pl.ds(pl.multiple_of(start * BLOCK, BLOCK), size * BLOCK)
            write(vis_ref.at[:, spot(group), columns], spot(group), columns)
            size //= 2
    for other in range(groups):
        gram[other] = acc[other] + product(planes[last, :, span], planes[other, :, span])
    for other in range(groups):
        vis_re, vis_im = weigh(gram[other], gcols[last], grows[other])
        row_strip[other, 0] = vis_re
        row_strip[other, 1] = vis_im
        write(row_strip.at[other], spot(last), spot(other))
        if other != last:
            column_strip[other, 0] = jnp.transpose(vis_re)
            column_strip[other, 1] = jnp.transpose(-vis_im)
            write(column_strip.at[other], spot(other), spot(last))
    for copy in copies:
        copy.wait()


def body(voltages, complex_gains, channel_map):
    n = lax.axis_size("feed")
    slots, rows, words = voltages.shape[1:]
    feeds = rows * n
    gains = complex_gains[:, 0]
    per_group = BLOCK // rows
    if per_group > 1:
        low = lax.rem(lax.axis_index("feed"), per_group)
        gains = lax.dynamic_update_slice(jnp.zeros((2, slots, BLOCK), gains.dtype), gains, (0, 0, low * rows))
    scale = 1.0 / (16.0 * words * 4)
    groups = feeds // BLOCK
    chunks = words // LANES
    pieces = 4 if rows % 32 == 0 else 1
    slices = max(chunks, pieces)
    dma = pltpu.SemaphoreType.DMA
    vmem = pl.BlockSpec(memory_space=pltpu.VMEM)
    hbm = pl.BlockSpec(memory_space=pltpu.HBM)
    held = pl.pallas_call(
        functools.partial(gather_kernel, n, scale),
        out_shape=[
            pltpu.VMEM((2, feeds, feeds), jnp.float32),
            pltpu.VMEM((groups, 2 * BLOCK, 4 * words), PLANE),
            pltpu.VMEM((groups, 2 * BLOCK, 2 * BLOCK), jnp.float32),
            pltpu.VMEM((groups, BLOCK, 8), jnp.float32),
            pltpu.VMEM((groups, 2, BLOCK), jnp.float32),
        ],
        in_specs=[hbm] * 3,
        out_specs=[vmem] * 5,
        scratch_shapes=[
            pltpu.SMEM((1, slots), jnp.int32),
            pltpu.VMEM((2, slots, BLOCK), jnp.float32),
            [pltpu.VMEM((slots, rows // pieces, words), jnp.int32)] * pieces,
            pltpu.VMEM((slots, rows, words), jnp.int32),
            pltpu.VMEM((slots, 2, BLOCK), jnp.float32),
            pltpu.VMEM((n, rows, words), jnp.int32),
            pltpu.VMEM((n, 2, BLOCK), jnp.float32),
            dma, dma, dma((pieces,)), dma((n, slices)), dma((n, slices)), dma((n,)), dma((n,)),
        ],
        compiler_params=pltpu.CompilerParams(
            collective_id=0, has_side_effects=True, vmem_limit_bytes=24 * 1024 * 1024),
    )(*[pltpu.with_memory_space_constraint(x, pltpu.HBM) for x in (channel_map, voltages, gains)])
    vis = pl.pallas_call(
        write_kernel,
        out_shape=jax.ShapeDtypeStruct((2, feeds, feeds), jnp.float32),
        in_specs=[vmem] * 5,
        out_specs=hbm,
        scratch_shapes=[
            pltpu.VMEM((groups, 2 * BLOCK, 2 * BLOCK), jnp.float32),
            pltpu.VMEM((groups, 2, BLOCK, BLOCK), jnp.float32),
            pltpu.VMEM((groups, 2, BLOCK, BLOCK), jnp.float32),
            dma((groups * groups,)),
        ],
        compiler_params=pltpu.CompilerParams(vmem_limit_bytes=16 * 1024 * 1024),
    )(*held)
    return vis[:, None, None]


def solution(mesh):
    in_specs = (P("band", None, "feed", None), P(None, "band", None, "feed"), P("band", None))
    out_specs = P(None, "band", "feed", None, None)
    return jax.shard_map(body, mesh=mesh, in_specs=in_specs, out_specs=out_specs, check_vma=False)
```

```python
import functools

import jax
import jax.numpy as jnp
from jax import lax
from jax.experimental import pallas as pl
from jax.experimental.pallas import tpu as pltpu
from jax.sharding import PartitionSpec as P

MESH = pl.DeviceIdType.MESH
PLANE = jnp.bfloat16
BLOCK = 128
LANES = 128


def flip(index, mask, size):
    total, bit = 0, 1
    while bit < size:
        digit = lax.rem(index // bit, 2)
        total = total + ((1 - digit) if mask & bit else digit) * bit
        bit *= 2
    return total


def weigh(gram, col, row):
    gram_re = gram[:BLOCK, :BLOCK] + gram[BLOCK:, BLOCK:]
    gram_im = gram[BLOCK:, :BLOCK] - gram[:BLOCK, BLOCK:]
    col_re, col_im = col[:, 0:1], col[:, 1:2]
    row_re, row_im = row[0:1, :], row[1:2, :]
    weight_re = col_re * row_re + col_im * row_im
    weight_im = col_im * row_re - col_re * row_im
    return weight_re * gram_re - weight_im * gram_im, weight_re * gram_im + weight_im * gram_re


def product(left, right):
    return lax.dot_general(left, right, (((1,), (1,)), ((), ())), preferred_element_type=jnp.float32)


def send_order(n):
    return sorted(range(1, n), key=lambda m: (m & (m - 1) > 1 and bin(m >> 1).count("1") > 1, m & 1, m))


def group_order(n, per_group):
    seen = []
    for mask in [0] + send_order(n):
        if mask // per_group not in seen:
            seen.append(mask // per_group)
    return seen


def gather_kernel(n, scale, map_hbm, volt_hbm, gain_hbm, vis_ref, planes, acc, gcols, grows,
                  map_ref, gain_ref, volts, stage, gstage, recv, grecv,
                  map_sem, gain_sem, load_sem, send_sem, recv_sem, gsend_sem, grecv_sem):
    me = lax.axis_index("feed")
    rows, words = stage.shape[1], stage.shape[2]
    per_group = BLOCK // rows
    groups = n // per_group
    chunks = words // LANES
    low = lax.rem(me, per_group)
    own_group = me // per_group
    arrivals = group_order(n, per_group)
    whole, chunked = arrivals[:-2], arrivals[-2:]
    last = chunked[-1]
    pieces = len(volts)
    step = rows // pieces

    map_copy = pltpu.make_async_copy(map_hbm, map_ref, map_sem)
    gain_copy = pltpu.make_async_copy(gain_hbm, gain_ref, gain_sem)
    loads = []
    for p in range(pieces):
        strip = pl.ds(p * step, step)
        loads.append(pltpu.make_async_copy(volt_hbm.at[0, :, strip], volts[p], load_sem.at[p]))
    map_copy.start()
    for load in loads:
        load.start()
    gain_copy.start()
    barrier = pltpu.get_barrier_semaphore()
    for mask in range(1, n):
        pl.semaphore_signal(barrier, inc=1, device_id={"feed": flip(me, mask, n)}, device_id_type=MESH)
    map_copy.wait()
    order = send_order(n)
    lead, rest = order[:2], order[2:]
    copies = []

    def send(source, target, sent, landed, mask):
        copies.append(pltpu.make_async_remote_copy(
            src_ref=source, dst_ref=target, send_sem=sent, recv_sem=landed,
            device_id={"feed": flip(me, mask, n)}, device_id_type=MESH))
        copies[-1].start()

    def spot(mask):
        return (mask // per_group) * per_group + low

    for p in range(pieces):
        strip = pl.ds(p * step, step)
        loads[p].wait()
        for mask in lead:
            stage[mask, strip] = volts[p][map_ref[0, flip(me, mask, n)]]
        if p == 0:
            pl.semaphore_wait(barrier, n - 1)
        for mask in lead:
            send(stage.at[mask, strip], recv.at[spot(mask), strip], send_sem.at[mask, p],
                 recv_sem.at[spot(mask), p], mask)
        if p == 0:
            gain_copy.wait()
            for mask in range(n):
                channel = map_ref[0, flip(me, mask, n)]
                for part in range(2):
                    gstage[mask, part:part + 1, :] = gain_ref[part, pl.ds(channel, 1), :]
            for mask in order:
                send(gstage.at[mask], grecv.at[spot(mask)], gsend_sem.at[mask], grecv_sem.at[spot(mask)], mask)
    for mask in rest:
        for p in range(pieces):
            stage[mask, pl.ds(p * step, step)] = volts[p][map_ref[0, flip(me, mask, n)]]
        if mask // per_group in whole:
            send(stage.at[mask], recv.at[spot(mask)], send_sem.at[mask, 0], recv_sem.at[spot(mask), 0], mask)
    for group in chunked:
        for c in range(chunks):
            part = pl.ds(c * LANES, LANES)
            for mask in rest:
                if mask // per_group == group:
                    send(stage.at[mask, :, part], recv.at[spot(mask), :, part], send_sem.at[mask, c],
                         recv_sem.at[spot(mask), c], mask)
    for p in range(pieces):
        recv[low, pl.ds(p * step, step)] = volts[p][map_ref[0, me]]
    grecv[low] = gstage[0]

    def places(group):
        return [group * per_group + flip(low, t, per_group) for t in range(per_group) if group or t]

    def arrive(group):
        for t in range(per_group):
            place = group * per_group + flip(low, t, per_group)
            if group * per_group + t in lead:
                for p in range(pieces):
                    here = recv.at[place, pl.ds(p * step, step)]
                    pltpu.make_async_copy(here, here, recv_sem.at[place, p]).wait()
            elif group or t:
                pltpu.make_async_copy(recv.at[place], recv.at[place], recv_sem.at[place, 0]).wait()

    def unpack(group, c):
        step = 32
        part_of = pl.ds(c * LANES, LANES)

        def piece(i, carry):
            start = pl.multiple_of(i * step, step)
            if rows >= step:
                packed = recv[group, pl.ds(start, step), part_of]
            else:
                first = group * per_group + i * (step // rows)
                packed = recv[pl.ds(first, step // rows), :, part_of].reshape(step, LANES)
            for k in range(4):
                for part in range(2):
                    field = jnp.right_shift(jnp.left_shift(packed, 28 - 8 * k - 4 * part), 28)
                    column = (4 * c + k) * LANES
                    planes[group, pl.ds(part * BLOCK + start, step), column:column + LANES] = (
                        field.astype(jnp.float32).astype(PLANE))
            return carry

        lax.fori_loop(0, BLOCK // step, piece, 0)

    def emit(group, other, gram):
        top = pl.multiple_of(flip(own_group, group, groups) * BLOCK, BLOCK)
        left = pl.multiple_of(flip(own_group, other, groups) * BLOCK, BLOCK)
        vis_re, vis_im = weigh(gram, gcols[group], grows[other])
        vis_ref[0, pl.ds(top, BLOCK), pl.ds(left, BLOCK)] = vis_re
        vis_ref[1, pl.ds(top, BLOCK), pl.ds(left, BLOCK)] = vis_im
        if other != group:
            vis_ref[0, pl.ds(left, BLOCK), pl.ds(top, BLOCK)] = jnp.transpose(vis_re)
            vis_ref[1, pl.ds(left, BLOCK), pl.ds(top, BLOCK)] = jnp.transpose(-vis_im)

    for group in range(groups):
        for place in places(group):
            pltpu.make_async_copy(grecv.at[place], grecv.at[place], grecv_sem.at[place]).wait()
        gains = grecv[group * per_group]
        for t in range(1, per_group):
            gains = gains + grecv[group * per_group + t]
        grows[group] = gains
        gcols[group] = jnp.transpose(jnp.concatenate([gains * scale] + [jnp.zeros_like(gains)] * 3, axis=0))

    for position, group in enumerate(whole):
        arrive(group)
        for c in range(chunks):
            unpack(group, c)
        for other in whole[:position + 1]:
            emit(group, other, product(planes[group], planes[other]))

    for group in chunked:
        others = arrivals[:arrivals.index(group) + 1]
        for c in range(chunks):
            for place in places(group):
                here = recv.at[place, :, pl.ds(c * LANES, LANES)]
                pltpu.make_async_copy(here, here, recv_sem.at[place, c]).wait()
            unpack(group, c)
            span = pl.ds(4 * c * LANES, 4 * LANES)
            if c < chunks - 1 or group != last:
                for other in others:
                    term = product(planes[group, :, span], planes[other, :, span])
                    gram = term if c == 0 else acc[other] + term
                    if c < chunks - 1:
                        acc[other] = gram
                    else:
                        emit(group, other, gram)

    for copy in copies:
        copy.wait_send()


def write_kernel(vis_ref, planes, acc, gcols, grows, out_hbm, gram, row_strip, column_strip, sems):
    groups = planes.shape[0]
    per_group = lax.axis_size("feed") // groups
    own_group = lax.axis_index("feed") // per_group
    last = group_order(lax.axis_size("feed"), per_group)[-1]
    span = pl.ds(planes.shape[2] - 4 * LANES, 4 * LANES)

    def spot(group):
        return pl.ds(pl.multiple_of(flip(own_group, group, groups) * BLOCK, BLOCK), BLOCK)

    copies = []

    def write(source, rows, columns):
        copies.append(pltpu.make_async_copy(source, out_hbm.at[:, rows, columns], sems.at[len(copies)]))
        copies[-1].start()

    for group in range(groups):
        if group == last:
            continue
        size = groups // 2
        while size:
            prefix = last // size * size ^ size
            start = flip(own_group, prefix, groups) // size * size
            columns = pl.ds(pl.multiple_of(start * BLOCK, BLOCK), size * BLOCK)
            write(vis_ref.at[:, spot(group), columns], spot(group), columns)
            size //= 2
    for other in range(groups):
        gram[other] = acc[other] + product(planes[last, :, span], planes[other, :, span])
    for other in range(groups):
        vis_re, vis_im = weigh(gram[other], gcols[last], grows[other])
        row_strip[other, 0] = vis_re
        row_strip[other, 1] = vis_im
        write(row_strip.at[other], spot(last), spot(other))
        if other != last:
            column_strip[other, 0] = jnp.transpose(vis_re)
            column_strip[other, 1] = jnp.transpose(-vis_im)
            write(column_strip.at[other], spot(other), spot(last))
    for copy in copies:
        copy.wait()


def body(voltages, complex_gains, channel_map):
    n = lax.axis_size("feed")
    slots, rows, words = voltages.shape[1:]
    feeds = rows * n
    gains = complex_gains[:, 0]
    per_group = BLOCK // rows
    if per_group > 1:
        low = lax.rem(lax.axis_index("feed"), per_group)
        gains = lax.dynamic_update_slice(jnp.zeros((2, slots, BLOCK), gains.dtype), gains, (0, 0, low * rows))
    scale = 1.0 / (16.0 * words * 4)
    groups = feeds // BLOCK
    chunks = words // LANES
    pieces = 4 if rows % 32 == 0 else 1
    slices = max(chunks, pieces)
    dma = pltpu.SemaphoreType.DMA
    vmem = pl.BlockSpec(memory_space=pltpu.VMEM)
    hbm = pl.BlockSpec(memory_space=pltpu.HBM)
    held = pl.pallas_call(
        functools.partial(gather_kernel, n, scale),
        out_shape=[
            pltpu.VMEM((2, feeds, feeds), jnp.float32),
            pltpu.VMEM((groups, 2 * BLOCK, 4 * words), PLANE),
            pltpu.VMEM((groups, 2 * BLOCK, 2 * BLOCK), jnp.float32),
            pltpu.VMEM((groups, BLOCK, 8), jnp.float32),
            pltpu.VMEM((groups, 2, BLOCK), jnp.float32),
        ],
        in_specs=[hbm] * 3,
        out_specs=[vmem] * 5,
        scratch_shapes=[
            pltpu.SMEM((1, slots), jnp.int32),
            pltpu.VMEM((2, slots, BLOCK), jnp.float32),
            [pltpu.VMEM((slots, rows // pieces, words), jnp.int32)] * pieces,
            pltpu.VMEM((slots, rows, words), jnp.int32),
            pltpu.VMEM((slots, 2, BLOCK), jnp.float32),
            pltpu.VMEM((n, rows, words), jnp.int32),
            pltpu.VMEM((n, 2, BLOCK), jnp.float32),
            dma, dma, dma((pieces,)), dma((n, slices)), dma((n, slices)), dma((n,)), dma((n,)),
        ],
        compiler_params=pltpu.CompilerParams(
            collective_id=0, has_side_effects=True, vmem_limit_bytes=24 * 1024 * 1024),
    )(*[pltpu.with_memory_space_constraint(x, pltpu.HBM) for x in (channel_map, voltages, gains)])
    vis = pl.pallas_call(
        write_kernel,
        out_shape=jax.ShapeDtypeStruct((2, feeds, feeds), jnp.float32),
        in_specs=[vmem] * 5,
        out_specs=hbm,
        scratch_shapes=[
            pltpu.VMEM((groups, 2 * BLOCK, 2 * BLOCK), jnp.float32),
            pltpu.VMEM((groups, 2, BLOCK, BLOCK), jnp.float32),
            pltpu.VMEM((groups, 2, BLOCK, BLOCK), jnp.float32),
            dma((groups * groups,)),
        ],
        compiler_params=pltpu.CompilerParams(vmem_limit_bytes=16 * 1024 * 1024),
    )(*held)
    return vis[:, None, None]


def solution(mesh):
    in_specs = (P("band", None, "feed", None), P(None, "band", None, "feed"), P("band", None))
    out_specs = P(None, "band", "feed", None, None)
    return jax.shard_map(body, mesh=mesh, in_specs=in_specs, out_specs=out_specs, check_vma=False)
```

```python
import functools

import jax
import jax.numpy as jnp
from jax import lax
from jax.experimental import pallas as pl
from jax.experimental.pallas import tpu as pltpu
from jax.sharding import PartitionSpec as P

MESH = pl.DeviceIdType.MESH
PLANE = jnp.bfloat16
BLOCK = 128
LANES = 128
TAIL = 3


def flip(index, mask, size):
    total, bit = 0, 1
    while bit < size:
        digit = lax.rem(index // bit, 2)
        total = total + ((1 - digit) if mask & bit else digit) * bit
        bit *= 2
    return total


def weigh(gram, col, row):
    gram_re = gram[:BLOCK, :BLOCK] + gram[BLOCK:, BLOCK:]
    gram_im = gram[BLOCK:, :BLOCK] - gram[:BLOCK, BLOCK:]
    col_re, col_im = col[:, 0:1], col[:, 1:2]
    row_re, row_im = row[0:1, :], row[1:2, :]
    weight_re = col_re * row_re + col_im * row_im
    weight_im = col_im * row_re - col_re * row_im
    return weight_re * gram_re - weight_im * gram_im, weight_re * gram_im + weight_im * gram_re


def product(left, right):
    return lax.dot_general(left, right, (((1,), (1,)), ((), ())), preferred_element_type=jnp.float32)


def send_order(n):
    return sorted(range(1, n), key=lambda m: (m & (m - 1) > 1 and bin(m >> 1).count("1") > 1, m & 1, m))


def group_order(n, per_group):
    seen = []
    for mask in [0] + send_order(n):
        if mask // per_group not in seen:
            seen.append(mask // per_group)
    return seen


def gather_kernel(n, scale, map_hbm, volt_hbm, gain_hbm, vis_ref, planes, acc, gcols, grows,
                  map_ref, gain_ref, volts, stage, gstage, recv, grecv,
                  map_sem, gain_sem, load_sem, send_sem, recv_sem, gsend_sem, grecv_sem):
    me = lax.axis_index("feed")
    rows, words = stage.shape[1], stage.shape[2]
    per_group = BLOCK // rows
    groups = n // per_group
    chunks = words // LANES
    low = lax.rem(me, per_group)
    own_group = me // per_group
    arrivals = group_order(n, per_group)
    whole, chunked = arrivals[:-2], arrivals[-2:]
    last = chunked[-1]
    pieces = len(volts)
    step = rows // pieces

    map_copy = pltpu.make_async_copy(map_hbm, map_ref, map_sem)
    gain_copy = pltpu.make_async_copy(gain_hbm, gain_ref, gain_sem)
    loads = []
    for p in range(pieces):
        strip = pl.ds(p * step, step)
        loads.append(pltpu.make_async_copy(volt_hbm.at[0, :, strip], volts[p], load_sem.at[p]))
    map_copy.start()
    for load in loads:
        load.start()
    gain_copy.start()
    barrier = pltpu.get_barrier_semaphore()
    for mask in range(1, n):
        pl.semaphore_signal(barrier, inc=1, device_id={"feed": flip(me, mask, n)}, device_id_type=MESH)
    map_copy.wait()
    order = send_order(n)
    lead, rest = order[:2], order[2:]
    copies = []

    def send(source, target, sent, landed, mask):
        copies.append(pltpu.make_async_remote_copy(
            src_ref=source, dst_ref=target, send_sem=sent, recv_sem=landed,
            device_id={"feed": flip(me, mask, n)}, device_id_type=MESH))
        copies[-1].start()

    def spot(mask):
        return (mask // per_group) * per_group + low

    for p in range(pieces):
        strip = pl.ds(p * step, step)
        loads[p].wait()
        for mask in lead:
            stage[mask, strip] = volts[p][map_ref[0, flip(me, mask, n)]]
        if p == 0:
            pl.semaphore_wait(barrier, n - 1)
        for mask in lead:
            send(stage.at[mask, strip], recv.at[spot(mask), strip], send_sem.at[mask, p],
                 recv_sem.at[spot(mask), p], mask)
        if p == 0:
            gain_copy.wait()
            for mask in range(n):
                channel = map_ref[0, flip(me, mask, n)]
                for part in range(2):
                    gstage[mask, part:part + 1, :] = gain_ref[part, pl.ds(channel, 1), :]
            for mask in order:
                send(gstage.at[mask], grecv.at[spot(mask)], gsend_sem.at[mask], grecv_sem.at[spot(mask)], mask)
    for mask in rest:
        for p in range(pieces):
            stage[mask, pl.ds(p * step, step)] = volts[p][map_ref[0, flip(me, mask, n)]]
        if mask // per_group in whole:
            send(stage.at[mask], recv.at[spot(mask)], send_sem.at[mask, 0], recv_sem.at[spot(mask), 0], mask)
    for group in chunked:
        for c in range(chunks):
            part = pl.ds(c * LANES, LANES)
            for mask in rest:
                if mask // per_group == group:
                    send(stage.at[mask, :, part], recv.at[spot(mask), :, part], send_sem.at[mask, c],
                         recv_sem.at[spot(mask), c], mask)
    for p in range(pieces):
        recv[low, pl.ds(p * step, step)] = volts[p][map_ref[0, me]]
    grecv[low] = gstage[0]

    def places(group):
        return [group * per_group + flip(low, t, per_group) for t in range(per_group) if group or t]

    def arrive(group):
        for t in range(per_group):
            place = group * per_group + flip(low, t, per_group)
            if group * per_group + t in lead:
                for p in range(pieces):
                    here = recv.at[place, pl.ds(p * step, step)]
                    pltpu.make_async_copy(here, here, recv_sem.at[place, p]).wait()
            elif group or t:
                pltpu.make_async_copy(recv.at[place], recv.at[place], recv_sem.at[place, 0]).wait()

    def unpack(group, c):
        step = 32
        part_of = pl.ds(c * LANES, LANES)

        def piece(i, carry):
            start = pl.multiple_of(i * step, step)
            if rows >= step:
                packed = recv[group, pl.ds(start, step), part_of]
            else:
                first = group * per_group + i * (step // rows)
                packed = recv[pl.ds(first, step // rows), :, part_of].reshape(step, LANES)
            for k in range(4):
                for part in range(2):
                    field = jnp.right_shift(jnp.left_shift(packed, 28 - 8 * k - 4 * part), 28)
                    column = (4 * c + k) * LANES
                    planes[group, pl.ds(part * BLOCK + start, step), column:column + LANES] = (
                        field.astype(jnp.float32).astype(PLANE))
            return carry

        lax.fori_loop(0, BLOCK // step, piece, 0)

    def emit(group, other, gram):
        top = pl.multiple_of(flip(own_group, group, groups) * BLOCK, BLOCK)
        left = pl.multiple_of(flip(own_group, other, groups) * BLOCK, BLOCK)
        vis_re, vis_im = weigh(gram, gcols[group], grows[other])
        vis_ref[0, pl.ds(top, BLOCK), pl.ds(left, BLOCK)] = vis_re
        vis_ref[1, pl.ds(top, BLOCK), pl.ds(left, BLOCK)] = vis_im
        if other != group:
            vis_ref[0, pl.ds(left, BLOCK), pl.ds(top, BLOCK)] = jnp.transpose(vis_re)
            vis_ref[1, pl.ds(left, BLOCK), pl.ds(top, BLOCK)] = jnp.transpose(-vis_im)

    for group in range(groups):
        for place in places(group):
            pltpu.make_async_copy(grecv.at[place], grecv.at[place], grecv_sem.at[place]).wait()
        gains = grecv[group * per_group]
        for t in range(1, per_group):
            gains = gains + grecv[group * per_group + t]
        grows[group] = gains
        gcols[group] = jnp.transpose(jnp.concatenate([gains * scale] + [jnp.zeros_like(gains)] * 3, axis=0))

    for position, group in enumerate(whole):
        arrive(group)
        for c in range(chunks):
            unpack(group, c)
        for other in whole[:position + 1]:
            emit(group, other, product(planes[group], planes[other]))

    pair = max(chunks // 2, 1)
    for group in chunked:
        others = arrivals[:arrivals.index(group) + 1]
        for c in range(chunks):
            for place in places(group):
                here = recv.at[place, :, pl.ds(c * LANES, LANES)]
                pltpu.make_async_copy(here, here, recv_sem.at[place, c]).wait()
            unpack(group, c)
            if group == last:
                span = pl.ds(4 * c * LANES, 4 * LANES)
                if c < chunks - TAIL:
                    for other in others:
                        term = product(planes[group, :, span], planes[other, :, span])
                        acc[other] = term if c == 0 else acc[other] + term
            elif (c + 1) % pair == 0:
                span = pl.ds(4 * (c + 1 - pair) * LANES, 4 * pair * LANES)
                for other in others:
                    term = product(planes[group, :, span], planes[other, :, span])
                    gram = term if c + 1 == pair else acc[other] + term
                    if c < chunks - 1:
                        acc[other] = gram
                    else:
                        emit(group, other, gram)

    for copy in copies:
        copy.wait_send()


def write_kernel(vis_ref, planes, acc, gcols, grows, out_hbm, gram, row_strip, column_strip, sems):
    groups = planes.shape[0]
    per_group = lax.axis_size("feed") // groups
    own_group = lax.axis_index("feed") // per_group
    last = group_order(lax.axis_size("feed"), per_group)[-1]
    span = pl.ds(planes.shape[2] - 4 * TAIL * LANES, 4 * TAIL * LANES)

    def spot(group):
        return pl.ds(pl.multiple_of(flip(own_group, group, groups) * BLOCK, BLOCK), BLOCK)

    copies = []

    def write(source, rows, columns):
        copies.append(pltpu.make_async_copy(source, out_hbm.at[:, rows, columns], sems.at[len(copies)]))
        copies[-1].start()

    for group in range(groups):
        if group == last:
            continue
        size = groups // 2
        while size:
            prefix = last // size * size ^ size
            start = flip(own_group, prefix, groups) // size * size
            columns = pl.ds(pl.multiple_of(start * BLOCK, BLOCK), size * BLOCK)
            write(vis_ref.at[:, spot(group), columns], spot(group), columns)
            size //= 2
    for other in range(groups):
        gram[other] = acc[other] + product(planes[last, :, span], planes[other, :, span])
    for other in range(groups):
        vis_re, vis_im = weigh(gram[other], gcols[last], grows[other])
        row_strip[other, 0] = vis_re
        row_strip[other, 1] = vis_im
        write(row_strip.at[other], spot(last), spot(other))
        if other != last:
            column_strip[other, 0] = jnp.transpose(vis_re)
            column_strip[other, 1] = jnp.transpose(-vis_im)
            write(column_strip.at[other], spot(other), spot(last))
    for copy in copies:
        copy.wait()


def body(voltages, complex_gains, channel_map):
    n = lax.axis_size("feed")
    slots, rows, words = voltages.shape[1:]
    feeds = rows * n
    gains = complex_gains[:, 0]
    per_group = BLOCK // rows
    if per_group > 1:
        low = lax.rem(lax.axis_index("feed"), per_group)
        gains = lax.dynamic_update_slice(jnp.zeros((2, slots, BLOCK), gains.dtype), gains, (0, 0, low * rows))
    scale = 1.0 / (16.0 * words * 4)
    groups = feeds // BLOCK
    chunks = words // LANES
    pieces = 4 if rows % 32 == 0 else 1
    slices = max(chunks, pieces)
    dma = pltpu.SemaphoreType.DMA
    vmem = pl.BlockSpec(memory_space=pltpu.VMEM)
    hbm = pl.BlockSpec(memory_space=pltpu.HBM)
    held = pl.pallas_call(
        functools.partial(gather_kernel, n, scale),
        out_shape=[
            pltpu.VMEM((2, feeds, feeds), jnp.float32),
            pltpu.VMEM((groups, 2 * BLOCK, 4 * words), PLANE),
            pltpu.VMEM((groups, 2 * BLOCK, 2 * BLOCK), jnp.float32),
            pltpu.VMEM((groups, BLOCK, 8), jnp.float32),
            pltpu.VMEM((groups, 2, BLOCK), jnp.float32),
        ],
        in_specs=[hbm] * 3,
        out_specs=[vmem] * 5,
        scratch_shapes=[
            pltpu.SMEM((1, slots), jnp.int32),
            pltpu.VMEM((2, slots, BLOCK), jnp.float32),
            [pltpu.VMEM((slots, rows // pieces, words), jnp.int32)] * pieces,
            pltpu.VMEM((slots, rows, words), jnp.int32),
            pltpu.VMEM((slots, 2, BLOCK), jnp.float32),
            pltpu.VMEM((n, rows, words), jnp.int32),
            pltpu.VMEM((n, 2, BLOCK), jnp.float32),
            dma, dma, dma((pieces,)), dma((n, slices)), dma((n, slices)), dma((n,)), dma((n,)),
        ],
        compiler_params=pltpu.CompilerParams(
            collective_id=0, has_side_effects=True, vmem_limit_bytes=24 * 1024 * 1024),
    )(*[pltpu.with_memory_space_constraint(x, pltpu.HBM) for x in (channel_map, voltages, gains)])
    vis = pl.pallas_call(
        write_kernel,
        out_shape=jax.ShapeDtypeStruct((2, feeds, feeds), jnp.float32),
        in_specs=[vmem] * 5,
        out_specs=hbm,
        scratch_shapes=[
            pltpu.VMEM((groups, 2 * BLOCK, 2 * BLOCK), jnp.float32),
            pltpu.VMEM((groups, 2, BLOCK, BLOCK), jnp.float32),
            pltpu.VMEM((groups, 2, BLOCK, BLOCK), jnp.float32),
            dma((groups * groups,)),
        ],
        compiler_params=pltpu.CompilerParams(vmem_limit_bytes=16 * 1024 * 1024),
    )(*held)
    return vis[:, None, None]


def solution(mesh):
    in_specs = (P("band", None, "feed", None), P(None, "band", None, "feed"), P("band", None))
    out_specs = P(None, "band", "feed", None, None)
    return jax.shard_map(body, mesh=mesh, in_specs=in_specs, out_specs=out_specs, check_vma=False)
```

```python
import functools

import jax
import jax.numpy as jnp
from jax import lax
from jax.experimental import pallas as pl
from jax.experimental.pallas import tpu as pltpu
from jax.sharding import PartitionSpec as P

MESH = pl.DeviceIdType.MESH
PLANE = jnp.bfloat16
BLOCK = 128
LANES = 128
TAIL = 3


def flip(index, mask, size):
    total, bit = 0, 1
    while bit < size:
        digit = lax.rem(index // bit, 2)
        total = total + ((1 - digit) if mask & bit else digit) * bit
        bit *= 2
    return total


def weigh(gram, col, row):
    gram_re = gram[:BLOCK, :BLOCK] + gram[BLOCK:, BLOCK:]
    gram_im = gram[BLOCK:, :BLOCK] - gram[:BLOCK, BLOCK:]
    col_re, col_im = col[:, 0:1], col[:, 1:2]
    row_re, row_im = row[0:1, :], row[1:2, :]
    weight_re = col_re * row_re + col_im * row_im
    weight_im = col_im * row_re - col_re * row_im
    return weight_re * gram_re - weight_im * gram_im, weight_re * gram_im + weight_im * gram_re


def product(left, right):
    return lax.dot_general(left, right, (((1,), (1,)), ((), ())), preferred_element_type=jnp.float32)


def send_order(n):
    return sorted(range(1, n), key=lambda m: (m & (m - 1) > 1 and bin(m >> 1).count("1") > 1, m & 1, m))


def group_order(n, per_group):
    seen = []
    for mask in [0] + send_order(n):
        if mask // per_group not in seen:
            seen.append(mask // per_group)
    return seen


def gather_kernel(n, scale, map_hbm, volt_hbm, gain_hbm, vis_ref, planes, acc, gcols, grows,
                  map_ref, gain_ref, volts, stage, gstage, recv, grecv,
                  map_sem, gain_sem, load_sem, send_sem, whole_sem, half_sem, last_sem, gsend_sem, grecv_sem):
    me = lax.axis_index("feed")
    rows, words = stage.shape[1], stage.shape[2]
    per_group = BLOCK // rows
    groups = n // per_group
    chunks = words // LANES
    low = lax.rem(me, per_group)
    own_group = me // per_group
    arrivals = group_order(n, per_group)
    whole, chunked = arrivals[:-2], arrivals[-2:]
    last = chunked[-1]
    pieces = len(volts)
    step = rows // pieces

    map_copy = pltpu.make_async_copy(map_hbm, map_ref, map_sem)
    gain_copy = pltpu.make_async_copy(gain_hbm, gain_ref, gain_sem)
    loads = []
    for p in range(pieces):
        strip = pl.ds(p * step, step)
        loads.append(pltpu.make_async_copy(volt_hbm.at[0, :, strip], volts[p], load_sem.at[p]))
    map_copy.start()
    for load in loads:
        load.start()
    gain_copy.start()
    barrier = pltpu.get_barrier_semaphore()
    for mask in range(1, n):
        pl.semaphore_signal(barrier, inc=1, device_id={"feed": flip(me, mask, n)}, device_id_type=MESH)
    map_copy.wait()
    order = send_order(n)
    lead, rest = order[:2], order[2:]
    pair = max(chunks // 2, 1)

    def send(source, target, sent, landed, mask):
        pltpu.make_async_remote_copy(
            src_ref=source, dst_ref=target, send_sem=sent, recv_sem=landed,
            device_id={"feed": flip(me, mask, n)}, device_id_type=MESH).start()

    def landing(group, place, c):
        inner = place - group * per_group
        if group == last:
            return last_sem.at[inner, c]
        if group in chunked:
            return half_sem.at[inner, c // pair]
        return whole_sem.at[whole.index(group) * per_group + inner]

    def spot(mask):
        return (mask // per_group) * per_group + low

    for p in range(pieces):
        strip = pl.ds(p * step, step)
        loads[p].wait()
        for mask in lead:
            stage[mask, strip] = volts[p][map_ref[0, flip(me, mask, n)]]
        if p == 0:
            pl.semaphore_wait(barrier, n - 1)
        for mask in lead:
            send(stage.at[mask, strip], recv.at[spot(mask), strip], send_sem,
                 landing(mask // per_group, spot(mask), 0), mask)
        if p == 0:
            gain_copy.wait()
            for mask in range(n):
                channel = map_ref[0, flip(me, mask, n)]
                for part in range(2):
                    gstage[mask, part:part + 1, :] = gain_ref[part, pl.ds(channel, 1), :]
            for mask in order:
                send(gstage.at[mask], grecv.at[spot(mask)], gsend_sem, grecv_sem, mask)
    for mask in rest:
        for p in range(pieces):
            stage[mask, pl.ds(p * step, step)] = volts[p][map_ref[0, flip(me, mask, n)]]
        if mask // per_group in whole:
            send(stage.at[mask], recv.at[spot(mask)], send_sem, landing(mask // per_group, spot(mask), 0), mask)
    for group in chunked:
        for c in range(chunks):
            part = pl.ds(c * LANES, LANES)
            for mask in rest:
                if mask // per_group == group:
                    send(stage.at[mask, :, part], recv.at[spot(mask), :, part], send_sem,
                         landing(group, spot(mask), c), mask)
    for p in range(pieces):
        recv[low, pl.ds(p * step, step)] = volts[p][map_ref[0, me]]
    grecv[low] = gstage[0]

    def places(group):
        return [group * per_group + flip(low, t, per_group) for t in range(per_group) if group or t]

    def arrive(group):
        for place in places(group):
            pltpu.make_async_copy(recv.at[place], recv.at[place], landing(group, place, 0)).wait()

    def unpack(group, c):
        step = 32
        part_of = pl.ds(c * LANES, LANES)

        def piece(i, carry):
            start = pl.multiple_of(i * step, step)
            if rows >= step:
                packed = recv[group, pl.ds(start, step), part_of]
            else:
                first = group * per_group + i * (step // rows)
                packed = recv[pl.ds(first, step // rows), :, part_of].reshape(step, LANES)
            for k in range(4):
                for part in range(2):
                    field = jnp.right_shift(jnp.left_shift(packed, 28 - 8 * k - 4 * part), 28)
                    column = (4 * c + k) * LANES
                    planes[group, pl.ds(part * BLOCK + start, step), column:column + LANES] = (
                        field.astype(jnp.float32).astype(PLANE))
            return carry

        lax.fori_loop(0, BLOCK // step, piece, 0)

    def emit(group, other, gram):
        top = pl.multiple_of(flip(own_group, group, groups) * BLOCK, BLOCK)
        left = pl.multiple_of(flip(own_group, other, groups) * BLOCK, BLOCK)
        vis_re, vis_im = weigh(gram, gcols[group], grows[other])
        vis_ref[0, pl.ds(top, BLOCK), pl.ds(left, BLOCK)] = vis_re
        vis_ref[1, pl.ds(top, BLOCK), pl.ds(left, BLOCK)] = vis_im
        if other != group:
            vis_ref[0, pl.ds(left, BLOCK), pl.ds(top, BLOCK)] = jnp.transpose(vis_re)
            vis_ref[1, pl.ds(left, BLOCK), pl.ds(top, BLOCK)] = jnp.transpose(-vis_im)

    pltpu.make_async_copy(gstage.at[pl.ds(1, n - 1)], grecv.at[pl.ds(1, n - 1)], grecv_sem).wait()
    for group in range(groups):
        gains = grecv[group * per_group]
        for t in range(1, per_group):
            gains = gains + grecv[group * per_group + t]
        grows[group] = gains
        gcols[group] = jnp.transpose(jnp.concatenate([gains * scale] + [jnp.zeros_like(gains)] * 3, axis=0))

    for position, group in enumerate(whole):
        arrive(group)
        for c in range(chunks):
            unpack(group, c)
        for other in whole[:position + 1]:
            emit(group, other, product(planes[group], planes[other]))

    halved = chunked[0]
    others = arrivals[:-1]
    for h in range(chunks // pair):
        part = pl.ds(h * pair * LANES, pair * LANES)
        for place in places(halved):
            here = recv.at[place, :, part]
            pltpu.make_async_copy(here, here, landing(halved, place, h * pair)).wait()
        for c in range(h * pair, (h + 1) * pair):
            unpack(halved, c)
        span = pl.ds(4 * h * pair * LANES, 4 * pair * LANES)
        for other in others:
            term = product(planes[halved, :, span], planes[other, :, span])
            gram = term if h == 0 else acc[other] + term
            if h < chunks // pair - 1:
                acc[other] = gram
            else:
                emit(halved, other, gram)

    for c in range(chunks):
        for place in places(last):
            here = recv.at[place, :, pl.ds(c * LANES, LANES)]
            pltpu.make_async_copy(here, here, landing(last, place, c)).wait()
        unpack(last, c)
        span = pl.ds(4 * c * LANES, 4 * LANES)
        if c < chunks - TAIL:
            for other in arrivals:
                term = product(planes[last, :, span], planes[other, :, span])
                acc[other] = term if c == 0 else acc[other] + term

    pltpu.make_async_copy(stage.at[pl.ds(1, n - 1)], recv.at[pl.ds(1, n - 1)], send_sem).wait()
    pltpu.make_async_copy(gstage.at[pl.ds(1, n - 1)], grecv.at[pl.ds(1, n - 1)], gsend_sem).wait()


def write_kernel(vis_ref, planes, acc, gcols, grows, out_hbm, gram, row_strip, column_strip, sem):
    groups = planes.shape[0]
    per_group = lax.axis_size("feed") // groups
    own_group = lax.axis_index("feed") // per_group
    last = group_order(lax.axis_size("feed"), per_group)[-1]
    span = pl.ds(planes.shape[2] - 4 * TAIL * LANES, 4 * TAIL * LANES)

    def spot(group):
        return pl.ds(pl.multiple_of(flip(own_group, group, groups) * BLOCK, BLOCK), BLOCK)

    def write(source, rows, columns):
        pltpu.make_async_copy(source, out_hbm.at[:, rows, columns], sem).start()

    for group in range(groups):
        if group == last:
            continue
        size = groups // 2
        while size:
            prefix = last // size * size ^ size
            start = flip(own_group, prefix, groups) // size * size
            columns = pl.ds(pl.multiple_of(start * BLOCK, BLOCK), size * BLOCK)
            write(vis_ref.at[:, spot(group), columns], spot(group), columns)
            size //= 2
    for other in range(groups):
        gram[other] = acc[other] + product(planes[last, :, span], planes[other, :, span])
    for other in range(groups):
        vis_re, vis_im = weigh(gram[other], gcols[last], grows[other])
        row_strip[other, 0] = vis_re
        row_strip[other, 1] = vis_im
        write(row_strip.at[other], spot(last), spot(other))
        if other != last:
            column_strip[other, 0] = jnp.transpose(vis_re)
            column_strip[other, 1] = jnp.transpose(-vis_im)
            write(column_strip.at[other], spot(other), spot(last))
    pltpu.make_async_copy(vis_ref, out_hbm, sem).wait()


def body(voltages, complex_gains, channel_map):
    n = lax.axis_size("feed")
    slots, rows, words = voltages.shape[1:]
    feeds = rows * n
    gains = complex_gains[:, 0]
    per_group = BLOCK // rows
    if per_group > 1:
        low = lax.rem(lax.axis_index("feed"), per_group)
        gains = lax.dynamic_update_slice(jnp.zeros((2, slots, BLOCK), gains.dtype), gains, (0, 0, low * rows))
    scale = 1.0 / (16.0 * words * 4)
    groups = feeds // BLOCK
    chunks = words // LANES
    pieces = 4 if rows % 32 == 0 else 1
    dma = pltpu.SemaphoreType.DMA
    vmem = pl.BlockSpec(memory_space=pltpu.VMEM)
    hbm = pl.BlockSpec(memory_space=pltpu.HBM)
    held = pl.pallas_call(
        functools.partial(gather_kernel, n, scale),
        out_shape=[
            pltpu.VMEM((2, feeds, feeds), jnp.float32),
            pltpu.VMEM((groups, 2 * BLOCK, 4 * words), PLANE),
            pltpu.VMEM((groups, 2 * BLOCK, 2 * BLOCK), jnp.float32),
            pltpu.VMEM((groups, BLOCK, 8), jnp.float32),
            pltpu.VMEM((groups, 2, BLOCK), jnp.float32),
        ],
        in_specs=[hbm] * 3,
        out_specs=[vmem] * 5,
        scratch_shapes=[
            pltpu.SMEM((1, slots), jnp.int32),
            pltpu.VMEM((2, slots, BLOCK), jnp.float32),
            [pltpu.VMEM((slots, rows // pieces, words), jnp.int32)] * pieces,
            pltpu.VMEM((slots, rows, words), jnp.int32),
            pltpu.VMEM((slots, 2, BLOCK), jnp.float32),
            pltpu.VMEM((n, rows, words), jnp.int32),
            pltpu.VMEM((n, 2, BLOCK), jnp.float32),
            dma, dma, dma((pieces,)), dma, dma((n - 2 * per_group,)), dma((per_group, 2)),
            dma((per_group, chunks)), dma, dma,
        ],
        compiler_params=pltpu.CompilerParams(
            collective_id=0, has_side_effects=True, vmem_limit_bytes=24 * 1024 * 1024),
    )(*[pltpu.with_memory_space_constraint(x, pltpu.HBM) for x in (channel_map, voltages, gains)])
    vis = pl.pallas_call(
        write_kernel,
        out_shape=jax.ShapeDtypeStruct((2, feeds, feeds), jnp.float32),
        in_specs=[vmem] * 5,
        out_specs=hbm,
        scratch_shapes=[
            pltpu.VMEM((groups, 2 * BLOCK, 2 * BLOCK), jnp.float32),
            pltpu.VMEM((groups, 2, BLOCK, BLOCK), jnp.float32),
            pltpu.VMEM((groups, 2, BLOCK, BLOCK), jnp.float32),
            dma,
        ],
        compiler_params=pltpu.CompilerParams(vmem_limit_bytes=16 * 1024 * 1024),
    )(*held)
    return vis[:, None, None]


def solution(mesh):
    in_specs = (P("band", None, "feed", None), P(None, "band", None, "feed"), P("band", None))
    out_specs = P(None, "band", "feed", None, None)
    return jax.shard_map(body, mesh=mesh, in_specs=in_specs, out_specs=out_specs, check_vma=False)
```

```python
import functools

import jax
import jax.numpy as jnp
from jax import lax
from jax.experimental import pallas as pl
from jax.experimental.pallas import tpu as pltpu
from jax.sharding import PartitionSpec as P

MESH = pl.DeviceIdType.MESH
PLANE = jnp.bfloat16
BLOCK = 128
LANES = 128
TAIL = 2


def load_cuts(rows):
    return [0, rows // 8, rows // 2, rows] if rows % 64 == 0 else [0, rows]


def unpack_field(packed, k, part):
    field = jnp.right_shift(jnp.left_shift(packed, 28 - 8 * k - 4 * part), 28)
    return field.astype(jnp.float32).astype(PLANE)


def flip(index, mask, size):
    total, bit = 0, 1
    while bit < size:
        digit = lax.rem(index // bit, 2)
        total = total + ((1 - digit) if mask & bit else digit) * bit
        bit *= 2
    return total


def weigh(gram, col, row):
    gram_re = gram[:BLOCK, :BLOCK] + gram[BLOCK:, BLOCK:]
    gram_im = gram[BLOCK:, :BLOCK] - gram[:BLOCK, BLOCK:]
    col_re, col_im = col[:, 0:1], col[:, 1:2]
    row_re, row_im = row[0:1, :], row[1:2, :]
    weight_re = col_re * row_re + col_im * row_im
    weight_im = col_im * row_re - col_re * row_im
    return weight_re * gram_re - weight_im * gram_im, weight_re * gram_im + weight_im * gram_re


def product(left, right):
    return lax.dot_general(left, right, (((1,), (1,)), ((), ())), preferred_element_type=jnp.float32)


def send_order(n):
    return sorted(range(1, n), key=lambda m: (m & (m - 1) > 1 and bin(m >> 1).count("1") > 1, m & 1, m))


def group_order(n, per_group):
    seen = []
    for mask in [0] + send_order(n):
        if mask // per_group not in seen:
            seen.append(mask // per_group)
    return seen


def gather_kernel(n, scale, map_hbm, volt_hbm, gain_hbm, vis_ref, planes, acc, gcols, grows, held,
                  map_ref, gain_ref, volts, stage, gstage, recv, grecv,
                  map_sem, gain_sem, load_sem, send_sem, whole_sem, half_sem, last_sem, gsend_sem, grecv_sem):
    me = lax.axis_index("feed")
    rows, words = stage.shape[1], stage.shape[2]
    per_group = BLOCK // rows
    groups = n // per_group
    chunks = words // LANES
    low = lax.rem(me, per_group)
    own_group = me // per_group
    arrivals = group_order(n, per_group)
    whole, chunked = arrivals[:-2], arrivals[-2:]
    last = chunked[-1]
    cuts = load_cuts(rows)
    strips = [pl.ds(a, b - a) for a, b in zip(cuts, cuts[1:])]

    map_copy = pltpu.make_async_copy(map_hbm, map_ref, map_sem)
    gain_copy = pltpu.make_async_copy(gain_hbm, gain_ref, gain_sem)
    loads = [pltpu.make_async_copy(volt_hbm.at[0, :, strip], volts[p], load_sem.at[p])
             for p, strip in enumerate(strips)]
    loads[0].start()
    map_copy.start()
    barrier = pltpu.get_barrier_semaphore()
    for mask in range(1, n):
        pl.semaphore_signal(barrier, inc=1, device_id={"feed": flip(me, mask, n)}, device_id_type=MESH)
    for load in loads[1:]:
        load.start()
    gain_copy.start()
    map_copy.wait()
    order = send_order(n)
    lead, rest = order[:2], order[2:]
    pair = max(chunks // 2, 1)

    def send(source, target, sent, landed, mask):
        pltpu.make_async_remote_copy(
            src_ref=source, dst_ref=target, send_sem=sent, recv_sem=landed,
            device_id={"feed": flip(me, mask, n)}, device_id_type=MESH).start()

    def landing(group, place, c):
        inner = place - group * per_group
        if group == last:
            return last_sem.at[inner, c]
        if group in chunked:
            return half_sem.at[inner, c // pair]
        return whole_sem.at[whole.index(group) * per_group + inner]

    def spot(mask):
        return (mask // per_group) * per_group + low

    for p, strip in enumerate(strips):
        loads[p].wait()
        for mask in lead:
            stage[mask, strip] = volts[p][map_ref[0, flip(me, mask, n)]]
        if p == 0:
            pl.semaphore_wait(barrier, n - 1)
        for mask in lead:
            send(stage.at[mask, strip], recv.at[spot(mask), strip], send_sem,
                 landing(mask // per_group, spot(mask), 0), mask)
        if p == 0:
            gain_copy.wait()
            for mask in range(n):
                channel = map_ref[0, flip(me, mask, n)]
                for part in range(2):
                    gstage[mask, part:part + 1, :] = gain_ref[part, pl.ds(channel, 1), :]
            for mask in order:
                send(gstage.at[mask], grecv.at[spot(mask)], gsend_sem, grecv_sem, mask)
    for mask in rest:
        for p, strip in enumerate(strips):
            stage[mask, strip] = volts[p][map_ref[0, flip(me, mask, n)]]
        if mask // per_group in whole:
            send(stage.at[mask], recv.at[spot(mask)], send_sem, landing(mask // per_group, spot(mask), 0), mask)
    for group in chunked:
        for c in range(chunks):
            part = pl.ds(c * LANES, LANES)
            for mask in rest:
                if mask // per_group == group:
                    send(stage.at[mask, :, part], recv.at[spot(mask), :, part], send_sem,
                         landing(group, spot(mask), c), mask)
    for p, strip in enumerate(strips):
        recv[low, strip] = volts[p][map_ref[0, me]]
    grecv[low] = gstage[0]

    def places(group):
        return [group * per_group + flip(low, t, per_group) for t in range(per_group) if group or t]

    def arrive(group):
        for place in places(group):
            pltpu.make_async_copy(recv.at[place], recv.at[place], landing(group, place, 0)).wait()

    def unpack(group, c):
        step = 32
        part_of = pl.ds(c * LANES, LANES)

        def piece(i, carry):
            start = pl.multiple_of(i * step, step)
            if rows >= step:
                packed = recv[group, pl.ds(start, step), part_of]
            else:
                first = group * per_group + i * (step // rows)
                packed = recv[pl.ds(first, step // rows), :, part_of].reshape(step, LANES)
            for k in range(4):
                for part in range(2):
                    column = (4 * c + k) * LANES
                    planes[group, pl.ds(part * BLOCK + start, step), column:column + LANES] = (
                        unpack_field(packed, k, part))
            return carry

        lax.fori_loop(0, BLOCK // step, piece, 0)

    def emit(group, other, gram):
        top = pl.multiple_of(flip(own_group, group, groups) * BLOCK, BLOCK)
        left = pl.multiple_of(flip(own_group, other, groups) * BLOCK, BLOCK)
        vis_re, vis_im = weigh(gram, gcols[group], grows[other])
        vis_ref[0, pl.ds(top, BLOCK), pl.ds(left, BLOCK)] = vis_re
        vis_ref[1, pl.ds(top, BLOCK), pl.ds(left, BLOCK)] = vis_im
        if other != group:
            vis_ref[0, pl.ds(left, BLOCK), pl.ds(top, BLOCK)] = jnp.transpose(vis_re)
            vis_ref[1, pl.ds(left, BLOCK), pl.ds(top, BLOCK)] = jnp.transpose(-vis_im)

    pltpu.make_async_copy(gstage.at[pl.ds(1, n - 1)], grecv.at[pl.ds(1, n - 1)], grecv_sem).wait()
    for group in range(groups):
        gains = grecv[group * per_group]
        for t in range(1, per_group):
            gains = gains + grecv[group * per_group + t]
        grows[group] = gains
        gcols[group] = jnp.transpose(jnp.concatenate([gains * scale] + [jnp.zeros_like(gains)] * 3, axis=0))

    for position, group in enumerate(whole):
        arrive(group)
        for c in range(chunks):
            unpack(group, c)
        for other in whole[:position + 1]:
            emit(group, other, product(planes[group], planes[other]))

    halved = chunked[0]
    others = arrivals[:-1]
    for h in range(chunks // pair):
        part = pl.ds(h * pair * LANES, pair * LANES)
        for place in places(halved):
            here = recv.at[place, :, part]
            pltpu.make_async_copy(here, here, landing(halved, place, h * pair)).wait()
        for c in range(h * pair, (h + 1) * pair):
            unpack(halved, c)
        span = pl.ds(4 * h * pair * LANES, 4 * pair * LANES)
        for other in others:
            term = product(planes[halved, :, span], planes[other, :, span])
            gram = term if h == 0 else acc[other] + term
            if h < chunks // pair - 1:
                acc[other] = gram
            else:
                emit(halved, other, gram)

    for c in range(chunks):
        for place in places(last):
            here = recv.at[place, :, pl.ds(c * LANES, LANES)]
            pltpu.make_async_copy(here, here, landing(last, place, c)).wait()
        if c == chunks - 1:
            held[...] = recv[pl.ds(last * per_group, per_group), :, pl.ds(c * LANES, LANES)].reshape(BLOCK, LANES)
            break
        unpack(last, c)
        span = pl.ds(4 * c * LANES, 4 * LANES)
        if c < chunks - TAIL:
            for other in arrivals:
                term = product(planes[last, :, span], planes[other, :, span])
                acc[other] = term if c == 0 else acc[other] + term

    pltpu.make_async_copy(stage.at[pl.ds(1, n - 1)], recv.at[pl.ds(1, n - 1)], send_sem).wait()
    pltpu.make_async_copy(gstage.at[pl.ds(1, n - 1)], grecv.at[pl.ds(1, n - 1)], gsend_sem).wait()


def write_kernel(vis_ref, planes, acc, gcols, grows, held, out_hbm, tail, gram, row_strip, column_strip, sem):
    groups = planes.shape[0]
    per_group = lax.axis_size("feed") // groups
    own_group = lax.axis_index("feed") // per_group
    last = group_order(lax.axis_size("feed"), per_group)[-1]
    chunks = planes.shape[2] // (4 * LANES)
    middle = pl.ds(4 * max(chunks - TAIL, 0) * LANES, 4 * (min(TAIL, chunks) - 1) * LANES)
    end = pl.ds(4 * (chunks - 1) * LANES, 4 * LANES)

    def spot(group):
        return pl.ds(pl.multiple_of(flip(own_group, group, groups) * BLOCK, BLOCK), BLOCK)

    def write(source, rows, columns):
        pltpu.make_async_copy(source, out_hbm.at[:, rows, columns], sem).start()

    for group in range(groups):
        if group == last:
            continue
        size = groups // 2
        while size:
            prefix = last // size * size ^ size
            start = flip(own_group, prefix, groups) // size * size
            columns = pl.ds(pl.multiple_of(start * BLOCK, BLOCK), size * BLOCK)
            write(vis_ref.at[:, spot(group), columns], spot(group), columns)
            size //= 2
    for k in range(4):
        for part in range(2):
            tail[part * BLOCK:(part + 1) * BLOCK, k * LANES:(k + 1) * LANES] = unpack_field(held[...], k, part)
    for other in range(groups):
        right = tail[...] if other == last else planes[other, :, end]
        gram[other] = acc[other] + product(planes[last, :, middle], planes[other, :, middle]) + product(tail[...], right)
    for other in range(groups):
        vis_re, vis_im = weigh(gram[other], gcols[last], grows[other])
        row_strip[other, 0] = vis_re
        row_strip[other, 1] = vis_im
        write(row_strip.at[other], spot(last), spot(other))
        if other != last:
            column_strip[other, 0] = jnp.transpose(vis_re)
            column_strip[other, 1] = jnp.transpose(-vis_im)
            write(column_strip.at[other], spot(other), spot(last))
    pltpu.make_async_copy(vis_ref, out_hbm, sem).wait()


def body(voltages, complex_gains, channel_map):
    n = lax.axis_size("feed")
    slots, rows, words = voltages.shape[1:]
    feeds = rows * n
    gains = complex_gains[:, 0]
    per_group = BLOCK // rows
    if per_group > 1:
        low = lax.rem(lax.axis_index("feed"), per_group)
        gains = lax.dynamic_update_slice(jnp.zeros((2, slots, BLOCK), gains.dtype), gains, (0, 0, low * rows))
    scale = 1.0 / (16.0 * words * 4)
    groups = feeds // BLOCK
    chunks = words // LANES
    cuts = load_cuts(rows)
    dma = pltpu.SemaphoreType.DMA
    vmem = pl.BlockSpec(memory_space=pltpu.VMEM)
    hbm = pl.BlockSpec(memory_space=pltpu.HBM)
    held = pl.pallas_call(
        functools.partial(gather_kernel, n, scale),
        out_shape=[
            pltpu.VMEM((2, feeds, feeds), jnp.float32),
            pltpu.VMEM((groups, 2 * BLOCK, 4 * words), PLANE),
            pltpu.VMEM((groups, 2 * BLOCK, 2 * BLOCK), jnp.float32),
            pltpu.VMEM((groups, BLOCK, 8), jnp.float32),
            pltpu.VMEM((groups, 2, BLOCK), jnp.float32),
            pltpu.VMEM((BLOCK, LANES), jnp.int32),
        ],
        in_specs=[hbm] * 3,
        out_specs=[vmem] * 6,
        scratch_shapes=[
            pltpu.SMEM((1, slots), jnp.int32),
            pltpu.VMEM((2, slots, BLOCK), jnp.float32),
            [pltpu.VMEM((slots, b - a, words), jnp.int32) for a, b in zip(cuts, cuts[1:])],
            pltpu.VMEM((slots, rows, words), jnp.int32),
            pltpu.VMEM((slots, 2, BLOCK), jnp.float32),
            pltpu.VMEM((n, rows, words), jnp.int32),
            pltpu.VMEM((n, 2, BLOCK), jnp.float32),
            dma, dma, dma((len(cuts) - 1,)), dma, dma((n - 2 * per_group,)), dma((per_group, 2)),
            dma((per_group, chunks)), dma, dma,
        ],
        compiler_params=pltpu.CompilerParams(
            collective_id=0, has_side_effects=True, vmem_limit_bytes=24 * 1024 * 1024),
    )(*[pltpu.with_memory_space_constraint(x, pltpu.HBM) for x in (channel_map, voltages, gains)])
    vis = pl.pallas_call(
        write_kernel,
        out_shape=jax.ShapeDtypeStruct((2, feeds, feeds), jnp.float32),
        in_specs=[vmem] * 6,
        out_specs=hbm,
        scratch_shapes=[
            pltpu.VMEM((2 * BLOCK, 4 * LANES), PLANE),
            pltpu.VMEM((groups, 2 * BLOCK, 2 * BLOCK), jnp.float32),
            pltpu.VMEM((groups, 2, BLOCK, BLOCK), jnp.float32),
            pltpu.VMEM((groups, 2, BLOCK, BLOCK), jnp.float32),
            dma,
        ],
        compiler_params=pltpu.CompilerParams(vmem_limit_bytes=16 * 1024 * 1024),
    )(*held)
    return vis[:, None, None]


def solution(mesh):
    in_specs = (P("band", None, "feed", None), P(None, "band", None, "feed"), P("band", None))
    out_specs = P(None, "band", "feed", None, None)
    return jax.shard_map(body, mesh=mesh, in_specs=in_specs, out_specs=out_specs, check_vma=False)
```

```python
import functools

import jax
import jax.numpy as jnp
from jax import lax
from jax.experimental import pallas as pl
from jax.experimental.pallas import tpu as pltpu
from jax.sharding import PartitionSpec as P

MESH = pl.DeviceIdType.MESH
PLANE = jnp.bfloat16
BLOCK = 128
LANES = 128
TAIL = 2


def load_cuts(rows):
    return [0, rows // 8, rows // 2, rows] if rows % 64 == 0 else [0, rows]


def unpack_field(packed, k, part):
    field = jnp.right_shift(jnp.left_shift(packed, 28 - 8 * k - 4 * part), 28)
    return field.astype(jnp.float32).astype(PLANE)


def flip(index, mask, size):
    total, bit = 0, 1
    while bit < size:
        digit = lax.rem(index // bit, 2)
        total = total + ((1 - digit) if mask & bit else digit) * bit
        bit *= 2
    return total


def weigh(gram, col, row):
    gram_re = gram[:BLOCK, :BLOCK] + gram[BLOCK:, BLOCK:]
    gram_im = gram[BLOCK:, :BLOCK] - gram[:BLOCK, BLOCK:]
    col_re, col_im = col[:, 0:1], col[:, 1:2]
    row_re, row_im = row[0:1, :], row[1:2, :]
    weight_re = col_re * row_re + col_im * row_im
    weight_im = col_im * row_re - col_re * row_im
    return weight_re * gram_re - weight_im * gram_im, weight_re * gram_im + weight_im * gram_re


def product(left, right):
    return lax.dot_general(left, right, (((1,), (1,)), ((), ())), preferred_element_type=jnp.float32)


def send_order(n):
    return sorted(range(1, n), key=lambda m: (m & (m - 1) > 1 and bin(m >> 1).count("1") > 1, m & 1, m))


def group_order(n, per_group):
    seen = []
    for mask in [0] + send_order(n):
        if mask // per_group not in seen:
            seen.append(mask // per_group)
    return seen


def gather_kernel(n, scale, map_hbm, volt_hbm, gain_hbm, vis_ref, planes, acc, gcols, grows, held,
                  map_ref, gain_ref, volts, stage, gstage, recv, grecv,
                  map_sem, gain_sem, load_sem, send_sem, whole_sem, half_sem, last_sem, gsend_sem, grecv_sem):
    me = lax.axis_index("feed")
    rows, words = stage.shape[1], stage.shape[2]
    per_group = BLOCK // rows
    groups = n // per_group
    chunks = words // LANES
    low = lax.rem(me, per_group)
    own_group = me // per_group
    arrivals = group_order(n, per_group)
    whole, chunked = arrivals[:-2], arrivals[-2:]
    last = chunked[-1]
    cuts = load_cuts(rows)
    strips = [pl.ds(a, b - a) for a, b in zip(cuts, cuts[1:])]

    map_copy = pltpu.make_async_copy(map_hbm, map_ref, map_sem)
    gain_copy = pltpu.make_async_copy(gain_hbm, gain_ref, gain_sem)
    loads = [pltpu.make_async_copy(volt_hbm.at[0, :, strip], volts[p], load_sem.at[p])
             for p, strip in enumerate(strips)]
    loads[0].start()
    map_copy.start()
    barrier = pltpu.get_barrier_semaphore()
    for mask in range(1, n):
        pl.semaphore_signal(barrier, inc=1, device_id={"feed": flip(me, mask, n)}, device_id_type=MESH)
    for load in loads[1:]:
        load.start()
    gain_copy.start()
    map_copy.wait()
    order = send_order(n)
    lead, rest = order[:2], order[2:]
    pair = max(chunks // 2, 1)

    def send(source, target, sent, landed, mask):
        pltpu.make_async_remote_copy(
            src_ref=source, dst_ref=target, send_sem=sent, recv_sem=landed,
            device_id={"feed": flip(me, mask, n)}, device_id_type=MESH).start()

    def landing(group, place, c):
        inner = place - group * per_group
        if group == last:
            return last_sem.at[inner, c]
        if group in chunked:
            return half_sem.at[inner, c // pair]
        return whole_sem.at[whole.index(group) * per_group + inner]

    def spot(mask):
        return (mask // per_group) * per_group + low

    for p, strip in enumerate(strips):
        loads[p].wait()
        for mask in lead:
            stage[mask, strip] = volts[p][map_ref[0, flip(me, mask, n)]]
        if p == 0:
            pl.semaphore_wait(barrier, n - 1)
        for mask in lead:
            send(stage.at[mask, strip], recv.at[spot(mask), strip], send_sem,
                 landing(mask // per_group, spot(mask), 0), mask)
        if p == 0:
            gain_copy.wait()
            for mask in range(n):
                channel = map_ref[0, flip(me, mask, n)]
                for part in range(2):
                    gstage[mask, part:part + 1, :] = gain_ref[part, pl.ds(channel, 1), :]
            for mask in order:
                send(gstage.at[mask], grecv.at[spot(mask)], gsend_sem, grecv_sem, mask)
    for mask in rest:
        for p, strip in enumerate(strips):
            stage[mask, strip] = volts[p][map_ref[0, flip(me, mask, n)]]
    for mask in rest:
        if mask // per_group in whole:
            send(stage.at[mask], recv.at[spot(mask)], send_sem, landing(mask // per_group, spot(mask), 0), mask)
    for group in chunked:
        for c in range(chunks):
            part = pl.ds(c * LANES, LANES)
            for mask in rest:
                if mask // per_group == group:
                    send(stage.at[mask, :, part], recv.at[spot(mask), :, part], send_sem,
                         landing(group, spot(mask), c), mask)
    for p, strip in enumerate(strips):
        recv[low, strip] = volts[p][map_ref[0, me]]
    grecv[low] = gstage[0]

    def places(group):
        return [group * per_group + flip(low, t, per_group) for t in range(per_group) if group or t]

    def arrive(group):
        for place in places(group):
            pltpu.make_async_copy(recv.at[place], recv.at[place], landing(group, place, 0)).wait()

    def unpack(group, c):
        step = 32
        part_of = pl.ds(c * LANES, LANES)

        def piece(i, carry):
            start = pl.multiple_of(i * step, step)
            if rows == BLOCK:
                packed = recv[group, pl.ds(start, step), part_of]
            elif rows >= step:
                inner = pl.multiple_of(lax.rem(start, rows), step)
                packed = recv[group * per_group + start // rows, pl.ds(inner, step), part_of]
            else:
                first = group * per_group + i * (step // rows)
                packed = recv[pl.ds(first, step // rows), :, part_of].reshape(step, LANES)
            for k in range(4):
                for part in range(2):
                    column = (4 * c + k) * LANES
                    planes[group, pl.ds(part * BLOCK + start, step), column:column + LANES] = (
                        unpack_field(packed, k, part))
            return carry

        lax.fori_loop(0, BLOCK // step, piece, 0)

    def emit(group, other, gram):
        top = pl.multiple_of(flip(own_group, group, groups) * BLOCK, BLOCK)
        left = pl.multiple_of(flip(own_group, other, groups) * BLOCK, BLOCK)
        vis_re, vis_im = weigh(gram, gcols[group], grows[other])
        vis_ref[0, pl.ds(top, BLOCK), pl.ds(left, BLOCK)] = vis_re
        vis_ref[1, pl.ds(top, BLOCK), pl.ds(left, BLOCK)] = vis_im
        if other != group:
            vis_ref[0, pl.ds(left, BLOCK), pl.ds(top, BLOCK)] = jnp.transpose(vis_re)
            vis_ref[1, pl.ds(left, BLOCK), pl.ds(top, BLOCK)] = jnp.transpose(-vis_im)

    pltpu.make_async_copy(gstage.at[pl.ds(1, n - 1)], grecv.at[pl.ds(1, n - 1)], grecv_sem).wait()
    for group in range(groups):
        gains = grecv[group * per_group]
        for t in range(1, per_group):
            gains = gains + grecv[group * per_group + t]
        grows[group] = gains
        gcols[group] = jnp.transpose(jnp.concatenate([gains * scale] + [jnp.zeros_like(gains)] * 3, axis=0))

    for position, group in enumerate(whole):
        arrive(group)
        for c in range(chunks):
            unpack(group, c)
        for other in whole[:position + 1]:
            emit(group, other, product(planes[group], planes[other]))

    halved = chunked[0]
    others = arrivals[:-1]
    for h in range(chunks // pair):
        part = pl.ds(h * pair * LANES, pair * LANES)
        for place in places(halved):
            here = recv.at[place, :, part]
            pltpu.make_async_copy(here, here, landing(halved, place, h * pair)).wait()
        for c in range(h * pair, (h + 1) * pair):
            unpack(halved, c)
        span = pl.ds(4 * h * pair * LANES, 4 * pair * LANES)
        for other in others:
            term = product(planes[halved, :, span], planes[other, :, span])
            gram = term if h == 0 else acc[other] + term
            if h < chunks // pair - 1:
                acc[other] = gram
            else:
                emit(halved, other, gram)

    for c in range(chunks):
        for place in places(last):
            here = recv.at[place, :, pl.ds(c * LANES, LANES)]
            pltpu.make_async_copy(here, here, landing(last, place, c)).wait()
        if c == chunks - 1:
            held[...] = recv[pl.ds(last * per_group, per_group), :, pl.ds(c * LANES, LANES)].reshape(BLOCK, LANES)
            break
        unpack(last, c)
        span = pl.ds(4 * c * LANES, 4 * LANES)
        if c < chunks - TAIL:
            for other in arrivals:
                term = product(planes[last, :, span], planes[other, :, span])
                acc[other] = term if c == 0 else acc[other] + term

    pltpu.make_async_copy(stage.at[pl.ds(1, n - 1)], recv.at[pl.ds(1, n - 1)], send_sem).wait()
    pltpu.make_async_copy(gstage.at[pl.ds(1, n - 1)], grecv.at[pl.ds(1, n - 1)], gsend_sem).wait()


def write_kernel(vis_ref, planes, acc, gcols, grows, held, out_hbm, tail, gram, row_strip, column_strip, sem):
    groups = planes.shape[0]
    per_group = lax.axis_size("feed") // groups
    own_group = lax.axis_index("feed") // per_group
    last = group_order(lax.axis_size("feed"), per_group)[-1]
    chunks = planes.shape[2] // (4 * LANES)
    middle = pl.ds(4 * max(chunks - TAIL, 0) * LANES, 4 * (min(TAIL, chunks) - 1) * LANES)
    end = pl.ds(4 * (chunks - 1) * LANES, 4 * LANES)

    def spot(group):
        return pl.ds(pl.multiple_of(flip(own_group, group, groups) * BLOCK, BLOCK), BLOCK)

    def write(source, rows, columns):
        pltpu.make_async_copy(source, out_hbm.at[:, rows, columns], sem).start()

    for group in range(groups):
        if group == last:
            continue
        size = groups // 2
        while size:
            prefix = last // size * size ^ size
            start = flip(own_group, prefix, groups) // size * size
            columns = pl.ds(pl.multiple_of(start * BLOCK, BLOCK), size * BLOCK)
            write(vis_ref.at[:, spot(group), columns], spot(group), columns)
            size //= 2
    for k in range(4):
        for part in range(2):
            tail[part * BLOCK:(part + 1) * BLOCK, k * LANES:(k + 1) * LANES] = unpack_field(held[...], k, part)
    for other in range(groups):
        right = tail[...] if other == last else planes[other, :, end]
        gram[other] = acc[other] + product(planes[last, :, middle], planes[other, :, middle]) + product(tail[...], right)
    for other in range(groups):
        vis_re, vis_im = weigh(gram[other], gcols[last], grows[other])
        row_strip[other, 0] = vis_re
        row_strip[other, 1] = vis_im
        write(row_strip.at[other], spot(last), spot(other))
        if other != last:
            column_strip[other, 0] = jnp.transpose(vis_re)
            column_strip[other, 1] = jnp.transpose(-vis_im)
            write(column_strip.at[other], spot(other), spot(last))
    pltpu.make_async_copy(vis_ref, out_hbm, sem).wait()


def body(voltages, complex_gains, channel_map):
    n = lax.axis_size("feed")
    slots, rows, words = voltages.shape[1:]
    feeds = rows * n
    gains = complex_gains[:, 0]
    per_group = BLOCK // rows
    if per_group > 1:
        low = lax.rem(lax.axis_index("feed"), per_group)
        gains = lax.dynamic_update_slice(jnp.zeros((2, slots, BLOCK), gains.dtype), gains, (0, 0, low * rows))
    scale = 1.0 / (16.0 * words * 4)
    groups = feeds // BLOCK
    chunks = words // LANES
    cuts = load_cuts(rows)
    dma = pltpu.SemaphoreType.DMA
    vmem = pl.BlockSpec(memory_space=pltpu.VMEM)
    hbm = pl.BlockSpec(memory_space=pltpu.HBM)
    held = pl.pallas_call(
        functools.partial(gather_kernel, n, scale),
        out_shape=[
            pltpu.VMEM((2, feeds, feeds), jnp.float32),
            pltpu.VMEM((groups, 2 * BLOCK, 4 * words), PLANE),
            pltpu.VMEM((groups, 2 * BLOCK, 2 * BLOCK), jnp.float32),
            pltpu.VMEM((groups, BLOCK, 8), jnp.float32),
            pltpu.VMEM((groups, 2, BLOCK), jnp.float32),
            pltpu.VMEM((BLOCK, LANES), jnp.int32),
        ],
        in_specs=[hbm] * 3,
        out_specs=[vmem] * 6,
        scratch_shapes=[
            pltpu.SMEM((1, slots), jnp.int32),
            pltpu.VMEM((2, slots, BLOCK), jnp.float32),
            [pltpu.VMEM((slots, b - a, words), jnp.int32) for a, b in zip(cuts, cuts[1:])],
            pltpu.VMEM((slots, rows, words), jnp.int32),
            pltpu.VMEM((slots, 2, BLOCK), jnp.float32),
            pltpu.VMEM((n, rows, words), jnp.int32),
            pltpu.VMEM((n, 2, BLOCK), jnp.float32),
            dma, dma, dma((len(cuts) - 1,)), dma, dma((n - 2 * per_group,)), dma((per_group, 2)),
            dma((per_group, chunks)), dma, dma,
        ],
        compiler_params=pltpu.CompilerParams(
            collective_id=0, has_side_effects=True, vmem_limit_bytes=24 * 1024 * 1024),
    )(*[pltpu.with_memory_space_constraint(x, pltpu.HBM) for x in (channel_map, voltages, gains)])
    vis = pl.pallas_call(
        write_kernel,
        out_shape=jax.ShapeDtypeStruct((2, feeds, feeds), jnp.float32),
        in_specs=[vmem] * 6,
        out_specs=hbm,
        scratch_shapes=[
            pltpu.VMEM((2 * BLOCK, 4 * LANES), PLANE),
            pltpu.VMEM((groups, 2 * BLOCK, 2 * BLOCK), jnp.float32),
            pltpu.VMEM((groups, 2, BLOCK, BLOCK), jnp.float32),
            pltpu.VMEM((groups, 2, BLOCK, BLOCK), jnp.float32),
            dma,
        ],
        compiler_params=pltpu.CompilerParams(vmem_limit_bytes=16 * 1024 * 1024),
    )(*held)
    return vis[:, None, None]


def solution(mesh):
    in_specs = (P("band", None, "feed", None), P(None, "band", None, "feed"), P("band", None))
    out_specs = P(None, "band", "feed", None, None)
    return jax.shard_map(body, mesh=mesh, in_specs=in_specs, out_specs=out_specs, check_vma=False)
```

```python
import functools

import jax
import jax.numpy as jnp
from jax import lax
from jax.experimental import pallas as pl
from jax.experimental.pallas import tpu as pltpu
from jax.sharding import PartitionSpec as P

MESH = pl.DeviceIdType.MESH
PLANE = jnp.bfloat16
BLOCK = 128
LANES = 128
TAIL = 2


def load_cuts(rows):
    return [0, rows // 8, rows] if rows % 64 == 0 else [0, rows]


def unpack_field(packed, k, part):
    field = jnp.right_shift(jnp.left_shift(packed, 28 - 8 * k - 4 * part), 28)
    return field.astype(jnp.float32).astype(PLANE)


def flip(index, mask, size):
    total, bit = 0, 1
    while bit < size:
        digit = lax.rem(index // bit, 2)
        total = total + ((1 - digit) if mask & bit else digit) * bit
        bit *= 2
    return total


def weigh(gram, col, row):
    gram_re = gram[:BLOCK, :BLOCK] + gram[BLOCK:, BLOCK:]
    gram_im = gram[BLOCK:, :BLOCK] - gram[:BLOCK, BLOCK:]
    col_re, col_im = col[:, 0:1], col[:, 1:2]
    row_re, row_im = row[0:1, :], row[1:2, :]
    weight_re = col_re * row_re + col_im * row_im
    weight_im = col_im * row_re - col_re * row_im
    return weight_re * gram_re - weight_im * gram_im, weight_re * gram_im + weight_im * gram_re


def product(left, right):
    return lax.dot_general(left, right, (((1,), (1,)), ((), ())), preferred_element_type=jnp.float32)


def send_order(n):
    return sorted(range(1, n), key=lambda m: (m & (m - 1) > 1 and bin(m >> 1).count("1") > 1, m & 1, m))


def group_order(n, per_group):
    seen = []
    for mask in [0] + send_order(n):
        if mask // per_group not in seen:
            seen.append(mask // per_group)
    return seen


def gather_kernel(n, scale, map_hbm, volt_hbm, gain_hbm, vis_ref, planes, acc, gcols, grows, held,
                  map_ref, gain_ref, volts, stage, gstage, recv, grecv,
                  map_sem, gain_sem, load_sem, send_sem, whole_sem, half_sem, last_sem, gsend_sem, grecv_sem):
    me = lax.axis_index("feed")
    rows, words = stage.shape[1], stage.shape[2]
    per_group = BLOCK // rows
    groups = n // per_group
    chunks = words // LANES
    low = lax.rem(me, per_group)
    own_group = me // per_group
    arrivals = group_order(n, per_group)
    whole, chunked = arrivals[:-2], arrivals[-2:]
    last = chunked[-1]
    cuts = load_cuts(rows)
    strips = [pl.ds(a, b - a) for a, b in zip(cuts, cuts[1:])]

    map_copy = pltpu.make_async_copy(map_hbm, map_ref, map_sem)
    gain_copy = pltpu.make_async_copy(gain_hbm, gain_ref, gain_sem)
    loads = [pltpu.make_async_copy(volt_hbm.at[0, :, strip], volts[p], load_sem.at[p])
             for p, strip in enumerate(strips)]
    loads[0].start()
    map_copy.start()
    barrier = pltpu.get_barrier_semaphore()
    for mask in range(1, n):
        pl.semaphore_signal(barrier, inc=1, device_id={"feed": flip(me, mask, n)}, device_id_type=MESH)
    for load in loads[1:]:
        load.start()
    gain_copy.start()
    map_copy.wait()
    order = send_order(n)
    lead, rest = order[:2], order[2:]
    pair = max(chunks // 2, 1)
    own = 1 if per_group == 1 else 0

    def send(source, target, sent, landed, mask):
        pltpu.make_async_remote_copy(
            src_ref=source, dst_ref=target, send_sem=sent, recv_sem=landed,
            device_id={"feed": flip(me, mask, n)}, device_id_type=MESH).start()

    def landing(group, place, c):
        inner = place - group * per_group
        if group == last:
            return last_sem.at[inner, c]
        if group in chunked:
            return half_sem.at[inner, c // pair]
        return whole_sem.at[whole.index(group) * per_group + inner - own]

    def spot(mask):
        return (mask // per_group) * per_group + low

    for p, strip in enumerate(strips):
        loads[p].wait()
        for mask in lead:
            stage[mask, strip] = volts[p][map_ref[0, flip(me, mask, n)]]
        if p == 0:
            pl.semaphore_wait(barrier, n - 1)
        for mask in lead:
            send(stage.at[mask, strip], recv.at[spot(mask), strip], send_sem,
                 landing(mask // per_group, spot(mask), 0), mask)
        if p == 0:
            gain_copy.wait()
            for mask in range(n):
                channel = map_ref[0, flip(me, mask, n)]
                for part in range(2):
                    gstage[mask, part:part + 1, :] = gain_ref[part, pl.ds(channel, 1), :]
            for mask in order:
                send(gstage.at[mask], grecv.at[spot(mask)], gsend_sem, grecv_sem, mask)
    for mask in rest:
        for p, strip in enumerate(strips):
            stage[mask, strip] = volts[p][map_ref[0, flip(me, mask, n)]]
    for mask in rest:
        if mask // per_group in whole:
            send(stage.at[mask], recv.at[spot(mask)], send_sem, landing(mask // per_group, spot(mask), 0), mask)
    for group in chunked:
        width = 1 if group == last else pair
        for c in range(0, chunks, width):
            part = pl.ds(c * LANES, width * LANES)
            for mask in rest:
                if mask // per_group == group:
                    send(stage.at[mask, :, part], recv.at[spot(mask), :, part], send_sem,
                         landing(group, spot(mask), c), mask)
    for p, strip in enumerate(strips):
        recv[low, strip] = volts[p][map_ref[0, me]]
    grecv[low] = gstage[0]

    def places(group):
        return [group * per_group + flip(low, t, per_group) for t in range(per_group) if group or t]

    def arrive(group):
        for place in places(group):
            pltpu.make_async_copy(recv.at[place], recv.at[place], landing(group, place, 0)).wait()

    def unpack(group, c):
        step = 32
        part_of = pl.ds(c * LANES, LANES)

        def piece(i, carry):
            start = pl.multiple_of(i * step, step)
            if rows == BLOCK:
                packed = recv[group, pl.ds(start, step), part_of]
            elif rows >= step:
                inner = pl.multiple_of(lax.rem(start, rows), step)
                packed = recv[group * per_group + start // rows, pl.ds(inner, step), part_of]
            else:
                first = group * per_group + i * (step // rows)
                packed = recv[pl.ds(first, step // rows), :, part_of].reshape(step, LANES)
            for k in range(4):
                for part in range(2):
                    column = (4 * c + k) * LANES
                    planes[group, pl.ds(part * BLOCK + start, step), column:column + LANES] = (
                        unpack_field(packed, k, part))
            return carry

        lax.fori_loop(0, BLOCK // step, piece, 0)

    def emit(group, other, gram):
        top = pl.multiple_of(flip(own_group, group, groups) * BLOCK, BLOCK)
        left = pl.multiple_of(flip(own_group, other, groups) * BLOCK, BLOCK)
        vis_re, vis_im = weigh(gram, gcols[group], grows[other])
        vis_ref[0, pl.ds(top, BLOCK), pl.ds(left, BLOCK)] = vis_re
        vis_ref[1, pl.ds(top, BLOCK), pl.ds(left, BLOCK)] = vis_im
        if other != group:
            vis_ref[0, pl.ds(left, BLOCK), pl.ds(top, BLOCK)] = jnp.transpose(vis_re)
            vis_ref[1, pl.ds(left, BLOCK), pl.ds(top, BLOCK)] = jnp.transpose(-vis_im)

    pltpu.make_async_copy(gstage.at[pl.ds(1, n - 1)], grecv.at[pl.ds(1, n - 1)], grecv_sem).wait()
    for group in range(groups):
        gains = grecv[group * per_group]
        for t in range(1, per_group):
            gains = gains + grecv[group * per_group + t]
        grows[group] = gains
        gcols[group] = jnp.transpose(jnp.concatenate([gains * scale] + [jnp.zeros_like(gains)] * 3, axis=0))

    for position, group in enumerate(whole):
        arrive(group)
        for c in range(chunks):
            unpack(group, c)
        for other in whole[:position + 1]:
            emit(group, other, product(planes[group], planes[other]))

    halved = chunked[0]
    others = arrivals[:-1]
    for h in range(chunks // pair):
        part = pl.ds(h * pair * LANES, pair * LANES)
        for place in places(halved):
            here = recv.at[place, :, part]
            pltpu.make_async_copy(here, here, landing(halved, place, h * pair)).wait()
        for c in range(h * pair, (h + 1) * pair):
            unpack(halved, c)
        span = pl.ds(4 * h * pair * LANES, 4 * pair * LANES)
        for other in others:
            term = product(planes[halved, :, span], planes[other, :, span])
            gram = term if h == 0 else acc[other] + term
            if h < chunks // pair - 1:
                acc[other] = gram
            else:
                emit(halved, other, gram)

    for c in range(chunks):
        for place in places(last):
            here = recv.at[place, :, pl.ds(c * LANES, LANES)]
            pltpu.make_async_copy(here, here, landing(last, place, c)).wait()
        if c == chunks - 1:
            held[...] = recv[pl.ds(last * per_group, per_group), :, pl.ds(c * LANES, LANES)].reshape(BLOCK, LANES)
            break
        unpack(last, c)
        span = pl.ds(4 * c * LANES, 4 * LANES)
        if c < chunks - TAIL:
            for other in arrivals:
                term = product(planes[last, :, span], planes[other, :, span])
                acc[other] = term if c == 0 else acc[other] + term

    pltpu.make_async_copy(stage.at[pl.ds(1, n - 1)], recv.at[pl.ds(1, n - 1)], send_sem).wait()
    pltpu.make_async_copy(gstage.at[pl.ds(1, n - 1)], grecv.at[pl.ds(1, n - 1)], gsend_sem).wait()


def write_kernel(vis_ref, planes, acc, gcols, grows, held, out_hbm, tail, gram, row_strip, column_strip, sem):
    groups = planes.shape[0]
    per_group = lax.axis_size("feed") // groups
    own_group = lax.axis_index("feed") // per_group
    last = group_order(lax.axis_size("feed"), per_group)[-1]
    chunks = planes.shape[2] // (4 * LANES)
    middle = pl.ds(4 * max(chunks - TAIL, 0) * LANES, 4 * (min(TAIL, chunks) - 1) * LANES)
    end = pl.ds(4 * (chunks - 1) * LANES, 4 * LANES)

    def spot(group):
        return pl.ds(pl.multiple_of(flip(own_group, group, groups) * BLOCK, BLOCK), BLOCK)

    def write(source, rows, columns):
        pltpu.make_async_copy(source, out_hbm.at[:, rows, columns], sem).start()

    for group in range(groups):
        if group == last:
            continue
        size = groups // 2
        while size:
            prefix = last // size * size ^ size
            start = flip(own_group, prefix, groups) // size * size
            columns = pl.ds(pl.multiple_of(start * BLOCK, BLOCK), size * BLOCK)
            write(vis_ref.at[:, spot(group), columns], spot(group), columns)
            size //= 2
    for k in range(4):
        for part in range(2):
            tail[part * BLOCK:(part + 1) * BLOCK, k * LANES:(k + 1) * LANES] = unpack_field(held[...], k, part)
    for other in range(groups):
        right = tail[...] if other == last else planes[other, :, end]
        gram[other] = acc[other] + product(planes[last, :, middle], planes[other, :, middle]) + product(tail[...], right)
    for other in range(groups):
        vis_re, vis_im = weigh(gram[other], gcols[last], grows[other])
        row_strip[other, 0] = vis_re
        row_strip[other, 1] = vis_im
        write(row_strip.at[other], spot(last), spot(other))
        if other != last:
            column_strip[other, 0] = jnp.transpose(vis_re)
            column_strip[other, 1] = jnp.transpose(-vis_im)
            write(column_strip.at[other], spot(other), spot(last))
    pltpu.make_async_copy(vis_ref, out_hbm, sem).wait()


def body(voltages, complex_gains, channel_map):
    n = lax.axis_size("feed")
    slots, rows, words = voltages.shape[1:]
    feeds = rows * n
    gains = complex_gains[:, 0]
    per_group = BLOCK // rows
    if per_group > 1:
        low = lax.rem(lax.axis_index("feed"), per_group)
        gains = lax.dynamic_update_slice(jnp.zeros((2, slots, BLOCK), gains.dtype), gains, (0, 0, low * rows))
    scale = 1.0 / (16.0 * words * 4)
    groups = feeds // BLOCK
    chunks = words // LANES
    cuts = load_cuts(rows)
    dma = pltpu.SemaphoreType.DMA
    vmem = pl.BlockSpec(memory_space=pltpu.VMEM)
    hbm = pl.BlockSpec(memory_space=pltpu.HBM)
    held = pl.pallas_call(
        functools.partial(gather_kernel, n, scale),
        out_shape=[
            pltpu.VMEM((2, feeds, feeds), jnp.float32),
            pltpu.VMEM((groups, 2 * BLOCK, 4 * words), PLANE),
            pltpu.VMEM((groups, 2 * BLOCK, 2 * BLOCK), jnp.float32),
            pltpu.VMEM((groups, BLOCK, 8), jnp.float32),
            pltpu.VMEM((groups, 2, BLOCK), jnp.float32),
            pltpu.VMEM((BLOCK, LANES), jnp.int32),
        ],
        in_specs=[hbm] * 3,
        out_specs=[vmem] * 6,
        scratch_shapes=[
            pltpu.SMEM((1, slots), jnp.int32),
            pltpu.VMEM((2, slots, BLOCK), jnp.float32),
            [pltpu.VMEM((slots, b - a, words), jnp.int32) for a, b in zip(cuts, cuts[1:])],
            pltpu.VMEM((slots, rows, words), jnp.int32),
            pltpu.VMEM((slots, 2, BLOCK), jnp.float32),
            pltpu.VMEM((n, rows, words), jnp.int32),
            pltpu.VMEM((n, 2, BLOCK), jnp.float32),
            dma, dma, dma((len(cuts) - 1,)), dma, dma((n - 2 * per_group - (per_group == 1),)), dma((per_group, 2)),
            dma((per_group, chunks)), dma, dma,
        ],
        compiler_params=pltpu.CompilerParams(
            collective_id=0, has_side_effects=True, vmem_limit_bytes=24 * 1024 * 1024),
    )(*[pltpu.with_memory_space_constraint(x, pltpu.HBM) for x in (channel_map, voltages, gains)])
    vis = pl.pallas_call(
        write_kernel,
        out_shape=jax.ShapeDtypeStruct((2, feeds, feeds), jnp.float32),
        in_specs=[vmem] * 6,
        out_specs=hbm,
        scratch_shapes=[
            pltpu.VMEM((2 * BLOCK, 4 * LANES), PLANE),
            pltpu.VMEM((groups, 2 * BLOCK, 2 * BLOCK), jnp.float32),
            pltpu.VMEM((groups, 2, BLOCK, BLOCK), jnp.float32),
            pltpu.VMEM((groups, 2, BLOCK, BLOCK), jnp.float32),
            dma,
        ],
        compiler_params=pltpu.CompilerParams(vmem_limit_bytes=16 * 1024 * 1024),
    )(*held)
    return vis[:, None, None]


def solution(mesh):
    in_specs = (P("band", None, "feed", None), P(None, "band", None, "feed"), P("band", None))
    out_specs = P(None, "band", "feed", None, None)
    return jax.shard_map(body, mesh=mesh, in_specs=in_specs, out_specs=out_specs, check_vma=False)
```
